32 devices in a mesh: gx: 4 (over x, core), gy: 4 (over z), gz: 2 (over y).
Axes of the slice: x: 2, y: 2, z: 4, core: 2. Of those that a mesh axis runs over, the one named last changes fastest.
Arguments:
- fractions: float32 [4, 4, 2, 3, 256], P('gx', 'gy', 'gz'), may hold values from 0 to 1
- velocity: float32 [4, 4, 2, 3, 256], P('gx', 'gy', 'gz'), may hold values from -30 to 30
- charge: float32 [4, 4, 2, 256], P('gx', 'gy', 'gz'), may hold values from -1.5 to 1.5
- drude_charge: float32 [4, 4, 2, 256], P('gx', 'gy', 'gz'), may hold values from -2.2 to -0.8
- screening: float32 [4, 4, 2, 256], P('gx', 'gy', 'gz'), may hold values from 0.2 to 2
- labels: int32 [4, 4, 2, 256], P('gx', 'gy', 'gz'), may hold values from 0 to 255
- masses: float32 [4, 4, 2, 256], P('gx', 'gy', 'gz'), may hold values from 4 to 32
- counts: int32 [4, 4, 2], P('gx', 'gy', 'gz'), may hold values from 128 to 256, as said below
- leaving: int32 [4, 4, 2, 6, 16], P('gx', 'gy', 'gz'), may hold values from -1 to 255, as said below
Outputs:
- staying: float32 [4, 4, 2, 9, 256], P('gx', 'gy', 'gz')
- arrivals: float32 [4, 4, 2, 14, 96], P('gx', 'gy', 'gz')
The draws below stay inside these ranges and needn't reach their ends.
Inputs may be any that keep to these rules, and one draw needn't show every extreme that they name: `counts`: at least one box holds 256 atoms. `leaving`: entries name distinct live slots of their box, or are -1; in every box some face has all 16 entries used.
All inputs are finite; a program needn't handle non-finite values.
Results may differ from the reference program's by a relative error of at most 0.0003.
Values sent between devices are 32-bit elements; how exact they have to be, the bound alone decides.
No kernel may reach another device: no remote copies, remote signals or barrier semaphores. Data moves between devices by JAX's collectives and lax.ppermute only.
A program may use at most 64 MiB of HBM per device.

```python
import math
import jax
import jax.numpy as jnp
from jax import lax

SLOTS = 256
MOVE = 16
ITERS = 3
BX = 4
BY = 4
BZ = 2


def lattice_size():
    lattice = 1
    while lattice * lattice * lattice < SLOTS:
        lattice = lattice + 1
    return lattice


def draw_fractions(key, part):
    lattice = lattice_size()
    box_total = BX * BY * BZ
    subkeys = jax.random.split(jax.random.fold_in(key, 3), box_total)
    chosen = jax.vmap(lambda subkey: jax.random.permutation(subkey, lattice * lattice * lattice)[:SLOTS])(subkeys)
    cell_ids = jnp.stack([chosen // (lattice * lattice), chosen // lattice % lattice, chosen % lattice], axis=1)
    jitters = jax.random.uniform(jax.random.fold_in(key, 5), (box_total, 3, SLOTS), jnp.float32, -0.3, 0.3)
    values = (cell_ids.astype(jnp.float32) + 0.5 + jitters) / lattice
    return values.reshape((BX, BY, BZ, 3, SLOTS))


def box_counts(key):
    box_total = BX * BY * BZ
    root_key = jax.random.fold_in(key, 17)
    sampled = jax.random.randint(jax.random.fold_in(root_key, 1), (box_total,), SLOTS // 2, SLOTS + 1)
    fullest = jax.random.randint(jax.random.fold_in(root_key, 2), (), 0, box_total)
    return jnp.where(jnp.arange(box_total) == fullest, SLOTS, sampled).astype(jnp.int32)


def draw_counts(key, part):
    return box_counts(key).reshape((BX, BY, BZ))


def draw_leaving(key, part):
    box_total = BX * BY * BZ
    box_sizes = box_counts(key)
    root_key = jax.random.fold_in(key, 29)

    def one_box(subkey, box_count):
        shuffled = jax.random.permutation(subkey, SLOTS)
        ranked = shuffled[jnp.argsort(jnp.where(shuffled < box_count, 0, 1), stable=True)]
        return ranked[:6 * MOVE].reshape((6, MOVE))
    chosen = jax.vmap(one_box)(jax.random.split(jax.random.fold_in(root_key, 1), box_total), box_sizes)
    lengths = jax.random.randint(jax.random.fold_in(root_key, 2), (box_total, 6), MOVE // 3, MOVE + 1)
    fullest = jax.random.randint(jax.random.fold_in(root_key, 3), (box_total,), 0, 6)
    lengths = jnp.where(lax.broadcasted_iota(jnp.int32, (box_total, 6), 1) == fullest[:, None], MOVE, lengths)
    occupied = lax.broadcasted_iota(jnp.int32, (box_total, 6, MOVE), 2) < lengths[:, :, None]
    return jnp.where(occupied, chosen, -1).reshape((BX, BY, BZ, 6, MOVE)).astype(jnp.int32)


def plant(entries, stream_key, low, largest):
    longest = entries.shape.index(max(entries.shape))
    spots = []
    for shift in (0, 1):
        where = [jax.random.randint(jax.random.fold_in(stream_key, axis), (), 0, length) for axis, length in enumerate(entries.shape)]
        where[longest] = (where[longest] + shift) % entries.shape[longest]
        spots.append(tuple(where))
    return entries.at[spots[0]].set(low).at[spots[1]].set(largest)


def levels(key, shape, shards, low, largest):
    factor_of, own = 1.0, jax.random.fold_in(key, 6)
    for axis_at, parts in shards:
        draws = jnp.exp(jax.random.uniform(jax.random.fold_in(own, axis_at), (parts,), jnp.float32, low / len(shards), largest / len(shards)))
        factor_of = factor_of * jnp.repeat(draws, shape[axis_at] // parts).reshape([-1 if axis == axis_at else 1 for axis in range(len(shape))])
    return factor_of


def scatter_about(stream_key, extent, spread, reach, cuts=(), kind=jnp.bfloat16):
    entries = jax.random.normal(stream_key, extent, jnp.float32) * spread
    if len(cuts) > 0:
        entries = levels(stream_key, extent, cuts, -0.22, 0.18) * entries
    return jnp.clip(entries, min=-reach, max=reach).astype(kind)


def setup_inputs(seed: int = 0) -> dict:
    arg_keys = jax.random.split(jax.random.key(seed), 10)
    return {
        "fractions": draw_fractions(jax.random.fold_in(arg_keys[9], 71), 0),
        "velocity": scatter_about(arg_keys[1], (BX, BY, BZ, 3, SLOTS), 5.0, 30.0, ((0, 4), (1, 4), (2, 2)), jnp.float32),
        "charge": scatter_about(arg_keys[2], (BX, BY, BZ, SLOTS), 0.5, 1.5, ((0, 4), (1, 4), (2, 2)), jnp.float32),
        "drude_charge": jnp.clip(-2.2 + 1.40000004 * jax.random.uniform(arg_keys[3], (BX, BY, BZ, SLOTS), jnp.float32) ** levels(arg_keys[3], (BX, BY, BZ, SLOTS), ((0, 4), (1, 4), (2, 2)), -0.2, 0.2), -2.2, -0.8),
        "screening": jnp.clip(jnp.exp(math.log(2.0) - 2.3025851 * jax.random.uniform(arg_keys[4], (BX, BY, BZ, SLOTS), jnp.float32) ** levels(arg_keys[4], (BX, BY, BZ, SLOTS), ((0, 4), (1, 4), (2, 2)), -0.2, 0.2)), 0.2, 2.0),
        "labels": plant(jax.random.randint(arg_keys[5], (BX, BY, BZ, SLOTS), 0, SLOTS), jax.random.fold_in(arg_keys[5], 1), 0, SLOTS - 1).astype(jnp.int32),
        "masses": jnp.clip(jnp.exp(math.log(32.0) - 2.0794415 * jax.random.uniform(arg_keys[6], (BX, BY, BZ, SLOTS), jnp.float32) ** levels(arg_keys[6], (BX, BY, BZ, SLOTS), ((0, 4), (1, 4), (2, 2)), -0.2, 0.2)), 4.0, 32.0),
        "counts": draw_counts(jax.random.fold_in(arg_keys[9], 71), 0),
        "leaving": draw_leaving(jax.random.fold_in(arg_keys[9], 71), 0),
    }


CUTOFF = 12.0
DRUDE_GAIN = 0.3320636
KICK = 0.002 * 418.4 * 332.0636
TIMESTEP = 0.002
UNITS = ((1, 0, 0), (-1, 0, 0), (0, 1, 0), (0, -1, 0), (0, 0, 1), (0, 0, -1))

def box_length():
    return max(12.0, (10.0 * SLOTS) ** (1.0 / 3.0))

def block_terms(target, source, moments, offset, same_box, charges, dipoles):
    length = box_length()
    slot_count = target.shape[-1]
    deltas = [(target[dimension][:, None] - source[dimension][None, :] - offset[dimension]) * length for dimension in range(3)]
    dist_sq = deltas[0] * deltas[0] + deltas[1] * deltas[1] + deltas[2] * deltas[2]
    row_ids = lax.broadcasted_iota(jnp.int32, (slot_count, slot_count), 0)
    col_ids = lax.broadcasted_iota(jnp.int32, (slot_count, slot_count), 1)
    itself = jnp.logical_and(same_box, row_ids == col_ids)
    dist_sq = jnp.where(itself, 1.0, dist_sq)
    inside = jnp.logical_and(dist_sq < CUTOFF * CUTOFF, jnp.logical_not(itself))
    switch = jnp.where(inside, jnp.square(1.0 - dist_sq / (CUTOFF * CUTOFF)), 0.0)
    inverse = lax.rsqrt(dist_sq)
    radial = switch * inverse * inverse * inverse
    alpha_target = DRUDE_GAIN * target[4] * target[4]
    alpha_source = DRUDE_GAIN * source[4] * source[4]
    damping = 0.5 * (target[5][:, None] + source[5][None, :]) * lax.rsqrt(alpha_target[:, None] * alpha_source[None, :])
    exponent = damping * dist_sq * jnp.sqrt(dist_sq)
    screen_three = -jnp.expm1(-exponent)
    screen_five = screen_three - exponent * jnp.exp(-exponent)
    fields = [jnp.zeros((slot_count,), target.dtype) for dimension in range(3)]
    if charges:
        allowed = target[6][:, None] != source[6][None, :]
        weight = jnp.where(allowed, radial * screen_three * source[3][None, :], 0.0)
        fields = [fields[dimension] + lax.optimization_barrier(jnp.sum(weight * deltas[dimension], axis=1)) for dimension in range(3)]
    if dipoles:
        moment = [source[4] * moments[dimension] for dimension in range(3)]
        projected = deltas[0] * moment[0][None, :] + deltas[1] * moment[1][None, :] + deltas[2] * moment[2][None, :]
        dipolar = 3.0 * radial * screen_five * inverse * inverse * projected
        direct = radial * screen_three
        fields = [fields[dimension] + lax.optimization_barrier(jnp.sum(dipolar * deltas[dimension] - direct * moment[dimension][None, :], axis=1)) for dimension in range(3)]
    return jnp.stack(fields)

def grid_field(statics, moments, charges, dipoles):
    box_total = statics.shape[0] * statics.shape[1] * statics.shape[2]
    group_size = math.gcd(box_total, 8)
    layout = (box_total // group_size, group_size)
    targets = statics.reshape(layout + statics.shape[3:])
    summed = jnp.zeros(statics.shape[:3] + (3, statics.shape[-1]), statics.dtype)
    for shift_x in (-1, 0, 1):
        for shift_y in (-1, 0, 1):
            for shift_z in (-1, 0, 1):
                rolled = (-shift_x, -shift_y, -shift_z)
                sources = jnp.roll(statics, rolled, axis=(0, 1, 2)).reshape(layout + statics.shape[3:])
                source_moments = jnp.roll(moments, rolled, axis=(0, 1, 2)).reshape(layout + moments.shape[3:])
                offset = (float(shift_x), float(shift_y), float(shift_z))
                same_box = shift_x == 0 and shift_y == 0 and (shift_z == 0)

                def per_group(arrays, offset=offset, same_box=same_box):

                    def single(target_row, source_row, moment_row):
                        return block_terms(target_row, source_row, moment_row, offset, same_box, charges, dipoles)
                    return jax.vmap(single)(arrays[0], arrays[1], arrays[2])
                blocks = lax.map(per_group, (targets, sources, source_moments))
                summed = summed + blocks.reshape(summed.shape)
    return summed

def reference(fractions, velocity, charge, drude_charge, screening, labels, masses, counts, leaving):
    slot_ids = lax.broadcasted_iota(jnp.int32, charge.shape, 3)
    is_live = slot_ids < counts[..., None]
    charge_live = jnp.where(is_live, charge, 0.0)
    drude_live = jnp.where(is_live, drude_charge, -1.0)
    label_values = labels.astype(fractions.dtype)
    statics = jnp.concatenate([fractions, charge_live[..., None, :], drude_live[..., None, :], screening[..., None, :], label_values[..., None, :]], axis=3)
    permanent = grid_field(statics, statics[:, :, :, :3], True, False)
    fields = permanent
    shifts = jnp.zeros_like(fractions)
    for iteration in range(ITERS):
        shifts = jnp.where(is_live[..., None, :], DRUDE_GAIN * drude_live[..., None, :] * fields, 0.0)
        fields = permanent + grid_field(statics, shifts, False, True)
    velocity_new = velocity + KICK * charge_live[..., None, :] * fields / masses[..., None, :]
    fractions_new = fractions + TIMESTEP * velocity_new / box_length()
    members = leaving[..., None] == lax.broadcasted_iota(jnp.int32, leaving.shape + (SLOTS,), 5)
    departed = jnp.any(members, axis=(3, 4))
    remain = jnp.logical_and(is_live, jnp.logical_not(departed))
    staying = jnp.where(remain[..., None, :], jnp.concatenate([fractions_new, velocity_new, shifts], axis=3), 0.0)
    complete = jnp.concatenate([fractions_new, velocity_new, shifts, charge_live[..., None, :], drude_live[..., None, :], screening[..., None, :], label_values[..., None, :], masses[..., None, :]], axis=3)
    pieces = []
    for direction in range(6):
        heading = UNITS[direction]
        sources = jnp.roll(complete, heading, axis=(0, 1, 2))
        slot_lists = jnp.roll(leaving[:, :, :, direction, :], heading, axis=(0, 1, 2))
        present = slot_lists >= 0
        indices = jnp.broadcast_to(jnp.maximum(slot_lists, 0)[..., None, :], sources.shape[:3] + (14, slot_lists.shape[-1]))
        picked = jnp.take_along_axis(sources, indices, axis=4)
        picked = jnp.where(present[..., None, :], picked, 0.0)
        frame_moves = jnp.zeros((14,), picked.dtype).at[0:3].set(-jnp.array(heading, picked.dtype))
        picked = picked + frame_moves[:, None] * present[..., None, :].astype(picked.dtype)
        pieces.append(picked)
    arrivals = jnp.concatenate(pieces, axis=4)
    return (staying, arrivals)
```

```python
import itertools

import jax
import jax.numpy as jnp
import numpy as np
from jax import lax
from jax.experimental import pallas as pl
from jax.experimental.pallas import tpu as pltpu
from jax.sharding import PartitionSpec as P

ITERS = 3
CUTOFF = 12.0
DRUDE_GAIN = 0.3320636
KICK = 0.002 * 418.4 * 332.0636
TIMESTEP = 0.002
UNITS = ((1, 0, 0), (-1, 0, 0), (0, 1, 0), (0, -1, 0), (0, 0, 1), (0, 0, -1))
AXES = ("gx", "gy", "gz")
LANES = 128
CENTERS = ((0, 0, 0),) + tuple(tuple(-step for step in unit) for unit in UNITS)
MOMENT = 2.0 / CUTOFF**3
F32 = jnp.float32
HIGHEST = lax.Precision.HIGHEST
VMEM = pltpu.VMEM


def vmem():
    return pl.BlockSpec(memory_space=pltpu.VMEM)


def smem():
    return pl.BlockSpec(memory_space=pltpu.SMEM)


def anywhere():
    return pl.BlockSpec(memory_space=pltpu.HBM)


def box_length(slots):
    return max(12.0, (10.0 * slots) ** (1.0 / 3.0))


def axis_steps(count):
    return ((0, False), (1, True)) if count == 2 else ((-1, False), (0, False), (1, False))


def shell(sizes):
    return list(itertools.product(*[axis_steps(count) for count in sizes]))


def own_cell():
    return [lax.axis_index(axis) for axis in AXES]


def linear(cell, steps, sizes):
    value = 0
    for coordinate, step, count in zip(cell, steps, sizes):
        value = value * count + (coordinate + (step % count)) % count
    return value


def around(cell, center, boxes, sizes):
    return [linear(cell, [center[a] + box[a][0] for a in range(3)], sizes) for box in boxes]


def fill_table(table, cell, boxes, sizes):
    for g, center in enumerate(CENTERS):
        for n, place in enumerate(around(cell, center, boxes, sizes)):
            table[g * len(boxes) + n] = place


def row_dot(rows, hit):
    return jnp.dot(rows, hit, precision=HIGHEST, preferred_element_type=F32)


def pack_kernel(sizes, slots, moves):
    devices = int(np.prod(sizes))

    def kernel(*refs):
        count, inputs, (send, own), staged, sems = refs[0], refs[1:9], refs[9:11], refs[11:19], refs[19]
        copies = [pltpu.make_async_copy(inputs[i], staged[i], sems.at[i]) for i in range(8)]
        for copy in copies:
            copy.start()
        for copy in copies:
            copy.wait()
        frac, vel, charge, drude, screen, label, mass, leaving = staged
        cell = own_cell()
        lane = lax.broadcasted_iota(jnp.int32, (1, slots), 1)
        live = lane < count[0]
        fr = jnp.concatenate([frac[a] for a in range(3)], axis=0)
        ve = jnp.concatenate([vel[a] for a in range(3)], axis=0)
        q = jnp.where(live, charge[...], 0.0)
        qd = jnp.where(live, drude[...], -1.0)
        sc = screen[...]
        lb = label[...].astype(F32)
        ms = mass[...]
        lv = jnp.concatenate([leaving[k].astype(F32) for k in range(6)], axis=0)
        lv = jnp.concatenate([lv, jnp.full((2, moves), -1.0, F32)], axis=0)
        spread = (
            lax.broadcasted_iota(jnp.int32, (moves, LANES), 1) % moves
            == lax.broadcasted_iota(jnp.int32, (moves, LANES), 0)
        ).astype(F32)
        repeated = row_dot(lv, spread)
        slot_col = lax.broadcasted_iota(jnp.int32, (slots, LANES), 0).astype(F32)
        values = jnp.concatenate([ve, ms, jnp.zeros((4, slots), F32)], axis=0)
        field = lax.broadcasted_iota(jnp.int32, (8, LANES), 1) // moves - 1
        wanted = field == lax.broadcasted_iota(jnp.int32, (8, LANES), 0)
        first = lax.broadcasted_iota(jnp.int32, (1, LANES), 1) < moves
        departed = jnp.zeros((1, slots), F32)
        statics = jnp.concatenate([fr, q, qd, sc, lb, jnp.zeros((1, slots), F32)], axis=0)
        send[...] = jnp.broadcast_to(statics[None], (devices, 8, slots))
        ones = jnp.ones((8, LANES), jnp.bfloat16)
        for k, unit in enumerate(UNITS):
            hit = slot_col == repeated[k : k + 1]
            picked = row_dot(values, hit.astype(F32))
            row = jnp.sum(jnp.where(wanted, picked, 0.0), axis=0, keepdims=True)
            row = jnp.where(first, repeated[k : k + 1], row)
            side = (k % 2) * LANES
            send[linear(cell, unit, sizes), 7:8, side : side + LANES] = row
            departed = departed + lax.dot_general(
                ones,
                hit.astype(F32).astype(jnp.bfloat16),
                (((1,), (1,)), ((), ())),
                preferred_element_type=F32,
            )[0:1]
        alive = live.astype(F32)
        gain = jnp.where(live, DRUDE_GAIN * qd, 0.0)
        own[...] = jnp.concatenate(
            [fr, q, qd, sc, lb, ms, ve, alive, jnp.where(departed > 0.5, 0.0, alive)]
            + [MOMENT * (gain * qd), gain, KICK * q / ms],
            axis=0,
        )

    return kernel


def columns(rows):
    lanes = rows.shape[1]
    padded = jnp.concatenate([rows, jnp.zeros((LANES - rows.shape[0], lanes), F32)], axis=0)
    return padded.T


def derived(fr, qd, sc, length):
    root = (DRUDE_GAIN**-0.5) / jnp.abs(qd)
    return fr * length, root, (0.25 * CUTOFF**3) * sc * root


def target_of(block, length, count):
    rows = block.shape[0]
    wide = [jnp.broadcast_to(block[:, c : c + 1], (rows, LANES)) for c in range(count)]
    shifted = [{-1: wide[a] + length, 0: wide[a], 1: wide[a] - length} for a in range(3)]
    return wide, shifted


def reader(source, place, half, rows):
    lanes = slice(half * LANES, (half + 1) * LANES)
    return lambda c: jnp.broadcast_to(source[place, c : c + 1, lanes], (rows, LANES))


def offsets(wide, shifted, row, box, length):
    deltas = []
    for a in range(3):
        step, nearest = box[a]
        if nearest:
            raw = wide[a] - row(a)
            deltas.append(raw - jnp.where(raw > 0.0, length, -length))
        else:
            deltas.append(shifted[a][step] - row(a))
    return deltas


def norm(deltas):
    return deltas[0] * deltas[0] + deltas[1] * deltas[1] + deltas[2] * deltas[2]


def terms(wide, dist_sq, row):
    inverse = lax.rsqrt(dist_sq)
    fade = inverse * jnp.maximum(1.0 - dist_sq, 0.0)
    half_x = (wide[3] * row(5) + wide[4] * row(4)) * (dist_sq * (dist_sq * inverse))
    tanh = jnp.tanh(half_x)
    root = lax.rsqrt(1.0 + tanh)
    base = ((fade * fade) * inverse) * (root * root)
    return inverse, half_x, tanh, base


def charge_sum(fields, wide, deltas, direct, row):
    weight = jnp.where(wide[5] != row(6), direct, 0.0) * row(3)
    return [fields[a] + weight * deltas[a] for a in range(3)]


def is_center(box):
    return all(step == 0 for step, _ in box)


def rows_of(parts):
    return [jnp.sum(part.T, axis=0, keepdims=True) for part in parts]


def send_moments(send, moments, slots):
    rows = [m[:, h * LANES : (h + 1) * LANES] for m in moments for h in range(slots // LANES)]
    rows.append(jnp.zeros((send.shape[1] - len(rows), LANES), F32))
    block = jnp.concatenate(rows, axis=0)
    send[...] = jnp.broadcast_to(block[None], send.shape)


def charge_kernel(sizes, slots, tile):
    boxes = shell(sizes)
    length = box_length(slots) / CUTOFF

    def kernel(recv, own, source, cols, perm, send, acc):
        fr, root, part = derived(recv[:, 0:3, :], recv[:, 4:5, :], recv[:, 5:6, :], length)
        source[:, 0:3, :] = fr
        source[:, 3:4, :] = (2.0 / CUTOFF**2) * recv[:, 3:4, :]
        source[:, 4:5, :] = root
        source[:, 5:6, :] = part
        source[:, 6:8, :] = recv[:, 6:8, :]
        fr, root, part = derived(own[0:3], own[4:5], own[5:6], length)
        ident = lax.broadcasted_iota(jnp.int32, (1, slots), 1).astype(F32)
        cols[...] = columns(jnp.concatenate([fr, root, part, own[6:7], ident, ident], axis=0))
        places = around(own_cell(), CENTERS[0], boxes, sizes)

        def body(t, carry):
            at = pl.ds(pl.multiple_of(t * tile, tile), tile)
            wide, shifted = target_of(cols[at, :], length, 6)
            fields = [jnp.zeros((tile, LANES), F32)] * 3
            for n, box in enumerate(boxes):
                for half in range(slots // LANES):
                    row = reader(source, places[n], half, tile)
                    deltas = offsets(wide, shifted, row, box, length)
                    _, _, tanh, base = terms(wide, norm(deltas), row)
                    fields = charge_sum(fields, wide, deltas, base * tanh, row)
            for a in range(3):
                acc[a, at, :] = fields[a]
            return carry

        lax.fori_loop(0, slots // tile, body, 0)
        rows = rows_of([acc[a] for a in range(3)])
        perm[...] = jnp.concatenate(rows, axis=0)
        send_moments(send, [own[13:14] * row for row in rows], slots)

    return kernel


def tensor_kernel(sizes, slots, moves):
    boxes = shell(sizes)
    length = box_length(slots) / CUTOFF
    tile = moves
    near_tiles = slots // tile

    def kernel(recv, source, cols, pairs, arrive, hits, perm, cols_in, stage, acc, table, sems):
        cell = own_cell()
        fill_table(table, cell, boxes, sizes)
        lane = lax.broadcasted_iota(jnp.int32, (1, LANES), 1)
        origin = [linear(cell, [-step for step in unit], sizes) for unit in UNITS]
        extra = jnp.full((8, LANES), -1.0, F32)
        for k in range(6):
            side = (k % 2) * LANES
            row = recv[origin[k], 7:8, side : side + LANES]
            row = jnp.broadcast_to(row, (8, LANES))
            fields = [pltpu.roll(row, (k * moves - c * moves) % LANES, 1)[0:1] for c in range(5)]
            block = jnp.concatenate(fields + [extra[0:3]], axis=0)
            extra = jnp.where(lane // moves == k, block, extra)
        slot = extra[0:1]
        slot_col = lax.broadcasted_iota(jnp.int32, (slots, LANES), 0).astype(F32)
        hit = (slot_col == slot).astype(F32)
        hits[...] = hit
        got = jnp.zeros((8, LANES), F32)
        for k in range(6):
            got = jnp.where(lane // moves == k, row_dot(recv[origin[k]], hit), got)
        present = (slot >= 0.0).astype(F32)
        arrive[...] = jnp.concatenate([got[0:7], extra[4:5], extra[1:4], present, slot, extra[5:8]], axis=0)
        fr, root, part = derived(got[0:3], got[4:5] - (1.0 - present), got[5:6], length)
        cols_in[...] = columns(jnp.concatenate([fr, root, part, got[6:7], slot, slot], axis=0))

        def body(t, block, offset, charges):
            wide, shifted = target_of(block, length, 7)
            fields = [jnp.zeros((tile, LANES), F32)] * 3
            for n, box in enumerate(boxes):
                place = table[offset + n]
                for half in range(slots // LANES):
                    row = reader(source, place, half, tile)
                    deltas = offsets(wide, shifted, row, box, length)
                    dist_sq = norm(deltas)
                    keep = None
                    if is_center(box):
                        ids = lax.broadcasted_iota(jnp.int32, (tile, LANES), 1) + half * LANES
                        keep = wide[6] != ids.astype(F32)
                        dist_sq = jnp.where(keep, dist_sq, 1.0)
                    inverse, half_x, tanh, base = terms(wide, dist_sq, row)
                    direct = base * tanh
                    if charges:
                        fields = charge_sum(fields, wide, deltas, direct, row)
                    radial = (base * (3.0 * inverse)) * (inverse * (tanh - half_x * (1.0 - tanh)))
                    if keep is not None:
                        direct = jnp.where(keep, direct, 0.0)
                        radial = jnp.where(keep, radial, 0.0)
                    lanes = slice(n * slots + half * LANES, n * slots + (half + 1) * LANES)
                    stage[t, 0, :, lanes] = radial
                    stage[t, 1, :, lanes] = direct
            pltpu.make_async_copy(stage.at[t], pairs.at[t], sems.at[t]).start()
            return fields

        def near(t, carry):
            body(t, cols[pl.ds(pl.multiple_of(t * tile, tile), tile), :], 0, False)
            return carry

        def incoming(k, carry):
            at = pl.ds(pl.multiple_of(k * tile, tile), tile)
            fields = body(near_tiles + k, cols_in[at, :], (k + 1) * len(boxes), True)
            for a in range(3):
                acc[a, at, :] = fields[a]
            return carry

        acc[...] = jnp.zeros(acc.shape, F32)
        lax.fori_loop(0, near_tiles, near, 0)
        lax.fori_loop(0, 6, incoming, 0)
        perm[...] = jnp.concatenate(rows_of([acc[a] for a in range(3)]), axis=0)

        def settle(t, carry):
            pltpu.make_async_copy(stage.at[t], pairs.at[t], sems.at[t]).wait()
            return carry

        lax.fori_loop(0, near_tiles + 6, settle, 0)

    return kernel


def apply_tile(block, load, source, recv, place_of, boxes, slots, length):
    rows = block.shape[0]
    halves = slots // LANES
    wide, shifted = target_of(block, length, 3)
    fields = [jnp.zeros((rows, LANES), F32)] * 3
    for n, box in enumerate(boxes):
        place = place_of(n)
        for half in range(halves):
            lanes = slice(n * slots + half * LANES, n * slots + (half + 1) * LANES)
            mu = [
                jnp.broadcast_to(recv[place, a * halves + half : a * halves + half + 1, :], (rows, LANES))
                for a in range(3)
            ]
            deltas = offsets(wide, shifted, reader(source, place, half, rows), box, length)
            along = load(0, lanes) * (deltas[0] * mu[0] + deltas[1] * mu[1] + deltas[2] * mu[2])
            direct = load(1, lanes)
            fields = [fields[a] + (along * deltas[a] - direct * mu[a]) for a in range(3)]
    return fields


def induced_kernel(sizes, slots, tile, fetch):
    boxes = shell(sizes)
    length = box_length(slots) / CUTOFF
    tiles = slots // tile

    def kernel(recv, pairs, source, cols, own, perm, send, shift, *rest):
        if fetch:
            kept, acc, sems = rest

            def begin(t, carry):
                pltpu.make_async_copy(pairs.at[t], kept.at[t], sems.at[t]).start()
                return carry

            lax.fori_loop(0, tiles, begin, 0)
        else:
            (acc,) = rest
            kept = pairs
        places = around(own_cell(), CENTERS[0], boxes, sizes)

        def body(t, carry):
            if fetch:
                pltpu.make_async_copy(pairs.at[t], kept.at[t], sems.at[t]).wait()
            at = pl.ds(pl.multiple_of(t * tile, tile), tile)
            load = lambda which, lanes: kept[t, which, :, lanes]
            fields = apply_tile(cols[at, :], load, source, recv, lambda n: places[n], boxes, slots, length)
            for a in range(3):
                acc[a, at, :] = fields[a]
            return carry

        lax.fori_loop(0, tiles, body, 0)
        rows = rows_of([acc[a] for a in range(3)])
        rows = [rows[a] + perm[a : a + 1] for a in range(3)]
        shift[...] = jnp.concatenate([own[14:15] * row for row in rows], axis=0)
        send_moments(send, [own[13:14] * row for row in rows], slots)

    return kernel


def final_kernel(sizes, slots, moves):
    boxes = shell(sizes)
    tile = moves
    halves = slots // LANES
    tiles = slots // tile
    edge = box_length(slots)
    length = edge / CUTOFF

    def kernel(
        recv, pairs, far, source, cols, own, perm, shift, arrive, hits, perm_in, cols_in,
        staying, arrivals, acc, kept, table, out_stay, out_come, sems, out_sems,
    ):
        def begin(k, carry):
            pltpu.make_async_copy(far.at[tiles + k], kept.at[k], sems.at[k]).start()
            return carry

        lax.fori_loop(0, 6, begin, 0)
        cell = own_cell()
        fill_table(table, cell, boxes, sizes)
        acc[...] = jnp.zeros(acc.shape, F32)
        lane = lax.broadcasted_iota(jnp.int32, (1, LANES), 1)

        def body(t, carry):
            at = pl.ds(pl.multiple_of(t * tile, tile), tile)
            load = lambda which, lanes: pairs[t, which, :, lanes]
            fields = apply_tile(cols[at, :], load, source, recv, lambda n: table[n], boxes, slots, length)
            for a in range(3):
                acc[a, at, :] = fields[a]
            return carry

        lax.fori_loop(0, tiles, body, 0)

        def incoming(k, carry):
            pltpu.make_async_copy(far.at[tiles + k], kept.at[k], sems.at[k]).wait()
            at = pl.ds(pl.multiple_of(k * tile, tile), tile)
            load = lambda which, lanes: kept[k, which, :, lanes]
            place_of = lambda n: table[(k + 1) * len(boxes) + n]
            fields = apply_tile(cols_in[at, :], load, source, recv, place_of, boxes, slots, length)
            for a in range(3):
                acc[a, pl.ds(pl.multiple_of(slots + k * tile, tile), tile), :] = fields[a]
            return carry

        lax.fori_loop(0, 6, incoming, 0)
        sums = rows_of([acc[a] for a in range(3)])
        field = [sums[a][:, 0:slots] + perm[a : a + 1] for a in range(3)]
        remain = own[12:13] > 0.5
        fast = [own[8 + a : 9 + a] + own[15:16] * field[a] for a in range(3)]
        place = [own[a : a + 1] + TIMESTEP * fast[a] / edge for a in range(3)]
        drude = [shift[a : a + 1] for a in range(3)]
        for r, row in enumerate(place + fast + drude):
            out_stay[r] = jnp.where(remain, row, 0.0)
        first = pltpu.make_async_copy(out_stay, staying, out_sems.at[0])
        first.start()

        moment = jnp.zeros((8, LANES), F32)
        for k, unit in enumerate(UNITS):
            block = recv[linear(cell, [-step for step in unit], sizes)]
            both = [row_dot(block, hits[h * LANES : (h + 1) * LANES, :]) for h in range(halves)]
            one = [
                sum(both[h][a * halves + h : a * halves + h + 1] for h in range(halves)) for a in range(3)
            ]
            one = jnp.concatenate(one + [jnp.zeros((5, LANES), F32)], axis=0)
            moment = jnp.where(lane // moves == k, one, moment)
        present = arrive[11:12] > 0.5
        q = arrive[3:4]
        qd = arrive[4:5]
        mass = jnp.where(present, arrive[7:8], 1.0)
        gain = KICK * q / mass
        pull = [sums[a][:, slots : slots + LANES] + perm_in[a : a + 1] for a in range(3)]
        fast = [arrive[8 + a : 9 + a] + gain * pull[a] for a in range(3)]
        place = [arrive[a : a + 1] + TIMESTEP * fast[a] / edge for a in range(3)]
        for k, unit in enumerate(UNITS):
            for a in range(3):
                if unit[a]:
                    place[a] = place[a] - jnp.where(lane // moves == k, float(unit[a]), 0.0)
        safe = jnp.where(present, qd, -1.0) * MOMENT
        drude = [moment[a : a + 1] / safe for a in range(3)]
        record = place + fast + drude + [q, qd, arrive[5:6], arrive[6:7], mass]
        for r, row in enumerate(record):
            out_come[r] = jnp.where(present, row, 0.0)[:, 0 : 6 * moves]
        second = pltpu.make_async_copy(out_come, arrivals, out_sems.at[1])
        second.start()
        first.wait()
        second.wait()

    return kernel


def solution(mesh):
    sizes = tuple(mesh.shape[axis] for axis in AXES)
    devices = int(np.prod(sizes))
    count_boxes = len(shell(sizes))

    def local(fractions, velocity, charge, drude_charge, screening, labels, masses, counts, leaving):
        slots = charge.shape[-1]
        moves = leaving.shape[-1]
        tiles = slots // moves
        lanes = count_boxes * slots
        exchange = lambda block: lax.all_to_all(block, AXES, 0, 0)
        shape = lambda *dims: jax.ShapeDtypeStruct(dims, F32)
        hbm = lambda x: pltpu.with_memory_space_constraint(x, pltpu.HBM)
        moment_shape = (devices, 8, LANES)
        dma = pltpu.SemaphoreType.DMA

        def call(kernel, in_specs, outs, out_specs, scratch, flops, limit):
            return pl.pallas_call(
                kernel,
                in_specs=in_specs,
                out_shape=outs,
                out_specs=out_specs,
                scratch_shapes=scratch,
                compiler_params=pltpu.CompilerParams(vmem_limit_bytes=limit),
                cost_estimate=pl.CostEstimate(flops=flops, bytes_accessed=1 << 20, transcendentals=0),
            )

        flat = [
            fractions.reshape(3, 1, slots),
            velocity.reshape(3, 1, slots),
            charge.reshape(1, slots),
            drude_charge.reshape(1, slots),
            screening.reshape(1, slots),
            labels.reshape(1, slots),
            masses.reshape(1, slots),
            leaving.reshape(6, 1, moves),
        ]
        send, own = call(
            pack_kernel(sizes, slots, moves),
            [smem()] + [anywhere()] * 8,
            (shape(devices, 8, slots), shape(16, slots)),
            (vmem(), vmem()),
            [VMEM(array.shape, array.dtype) for array in flat] + [dma((8,))],
            1 << 20,
            8 << 20,
        )(counts.reshape(1), *[hbm(x) for x in flat])
        recv = exchange(send)
        source, cols, perm, moments = call(
            charge_kernel(sizes, slots, moves),
            [vmem()] * 2,
            (shape(devices, 8, slots), shape(slots, LANES), shape(3, slots), shape(*moment_shape)),
            (vmem(),) * 4,
            [VMEM((3, slots, LANES), F32)],
            1 << 25,
            8 << 20,
        )(recv, own)
        got = exchange(moments)
        pairs, arrive, hits, perm_in, cols_in = call(
            tensor_kernel(sizes, slots, moves),
            [vmem()] * 3,
            (
                pltpu.HBM((tiles + 6, 2, moves, lanes), F32),
                shape(16, LANES),
                shape(slots, LANES),
                shape(3, LANES),
                shape(LANES, LANES),
            ),
            (anywhere(),) + (vmem(),) * 4,
            [
                VMEM((tiles + 6, 2, moves, lanes), F32),
                VMEM((3, LANES, LANES), F32),
                pltpu.SMEM((len(CENTERS) * count_boxes,), jnp.int32),
                dma((tiles + 6,)),
            ],
            1 << 26,
            32 << 20,
        )(recv, source, cols)
        far = pairs
        acc = VMEM((3, slots, LANES), F32)
        for step in range(ITERS - 1):
            outs = (shape(*moment_shape), shape(3, slots))
            fetch = step == 0
            if fetch:
                outs = outs + (shape(tiles, 2, moves, lanes),)
            results = call(
                induced_kernel(sizes, slots, moves, fetch),
                [vmem(), anywhere() if fetch else vmem()] + [vmem()] * 4,
                outs,
                (vmem(),) * len(outs),
                [acc, dma((tiles,))] if fetch else [acc],
                1 << 24,
                4 << 20,
            )(got, hbm(pairs) if fetch else pairs, source, cols, own, perm)
            moments, shift = results[:2]
            if fetch:
                pairs = results[2]
            got = exchange(moments)
        staying, arrivals = call(
            final_kernel(sizes, slots, moves),
            [vmem(), vmem(), anywhere()] + [vmem()] * 9,
            (pltpu.HBM((9, 1, slots), F32), pltpu.HBM((14, 1, 6 * moves), F32)),
            (anywhere(), anywhere()),
            [
                VMEM((3, slots + LANES, LANES), F32),
                VMEM((6, 2, moves, lanes), F32),
                pltpu.SMEM((len(CENTERS) * count_boxes,), jnp.int32),
                VMEM((9, 1, slots), F32),
                VMEM((14, 1, 6 * moves), F32),
                dma((6,)),
                dma((2,)),
            ],
            1 << 24,
            16 << 20,
        )(got, pairs, hbm(far), source, cols, own, perm, shift, arrive, hits, perm_in, cols_in)
        return staying.reshape(1, 1, 1, 9, slots), arrivals.reshape(1, 1, 1, 14, 6 * moves)

    box = P("gx", "gy", "gz", None)
    rows = P("gx", "gy", "gz", None, None)
    return jax.shard_map(
        local,
        mesh=mesh,
        in_specs=(rows, rows, box, box, box, box, box, P("gx", "gy", "gz"), rows),
        out_specs=(rows, rows),
        check_vma=False,
    )
```

```python
import itertools

import jax
import jax.numpy as jnp
import numpy as np
from jax import lax
from jax.experimental import pallas as pl
from jax.experimental.pallas import tpu as pltpu
from jax.sharding import PartitionSpec as P

ITERS = 3
CUTOFF = 12.0
DRUDE_GAIN = 0.3320636
KICK = 0.002 * 418.4 * 332.0636
TIMESTEP = 0.002
UNITS = ((1, 0, 0), (-1, 0, 0), (0, 1, 0), (0, -1, 0), (0, 0, 1), (0, 0, -1))
AXES = ("gx", "gy", "gz")
LANES = 128
CENTERS = ((0, 0, 0),) + tuple(tuple(-step for step in unit) for unit in UNITS)
MOMENT = 2.0 / CUTOFF**3
F32 = jnp.float32
BF16 = jnp.bfloat16
HIGHEST = lax.Precision.HIGHEST
VMEM = pltpu.VMEM


def vmem():
    return pl.BlockSpec(memory_space=pltpu.VMEM)


def smem():
    return pl.BlockSpec(memory_space=pltpu.SMEM)


def anywhere():
    return pl.BlockSpec(memory_space=pltpu.HBM)


def box_length(slots):
    return max(12.0, (10.0 * slots) ** (1.0 / 3.0))


def axis_steps(count):
    return ((0, False), (1, True)) if count == 2 else ((-1, False), (0, False), (1, False))


def shell(sizes):
    return list(itertools.product(*[axis_steps(count) for count in sizes]))


def own_cell():
    return [lax.axis_index(axis) for axis in AXES]


def linear(cell, steps, sizes):
    value = 0
    for coordinate, step, count in zip(cell, steps, sizes):
        value = value * count + (coordinate + (step % count)) % count
    return value


def around(cell, center, boxes, sizes):
    return [linear(cell, [center[a] + box[a][0] for a in range(3)], sizes) for box in boxes]


def fill_table(table, cell, boxes, sizes):
    for g, center in enumerate(CENTERS):
        for n, place in enumerate(around(cell, center, boxes, sizes)):
            table[g * len(boxes) + n] = place


def row_dot(rows, hit):
    return jnp.dot(rows, hit, precision=HIGHEST, preferred_element_type=F32)


def pack_kernel(sizes, slots, moves):
    devices = int(np.prod(sizes))

    def kernel(*refs):
        count, inputs, (send, own), staged, sems = refs[0], refs[1:9], refs[9:11], refs[11:19], refs[19]
        copies = [pltpu.make_async_copy(inputs[i], staged[i], sems.at[i]) for i in range(8)]
        for copy in copies:
            copy.start()
        for copy in copies:
            copy.wait()
        frac, vel, charge, drude, screen, label, mass, leaving = staged
        cell = own_cell()
        lane = lax.broadcasted_iota(jnp.int32, (1, slots), 1)
        live = lane < count[0]
        fr = jnp.concatenate([frac[a] for a in range(3)], axis=0)
        ve = jnp.concatenate([vel[a] for a in range(3)], axis=0)
        q = jnp.where(live, charge[...], 0.0)
        qd = jnp.where(live, drude[...], -1.0)
        sc = screen[...]
        lb = label[...].astype(F32)
        ms = mass[...]
        lv = jnp.concatenate([leaving[k].astype(F32) for k in range(6)], axis=0)
        lv = jnp.concatenate([lv, jnp.full((2, moves), -1.0, F32)], axis=0)
        spread = (
            lax.broadcasted_iota(jnp.int32, (moves, LANES), 1) % moves
            == lax.broadcasted_iota(jnp.int32, (moves, LANES), 0)
        ).astype(F32)
        repeated = row_dot(lv, spread)
        slot_col = lax.broadcasted_iota(jnp.int32, (slots, LANES), 0).astype(F32)
        values = jnp.concatenate([ve, ms, jnp.zeros((4, slots), F32)], axis=0)
        field = lax.broadcasted_iota(jnp.int32, (8, LANES), 1) // moves - 1
        wanted = field == lax.broadcasted_iota(jnp.int32, (8, LANES), 0)
        first = lax.broadcasted_iota(jnp.int32, (1, LANES), 1) < moves
        departed = jnp.zeros((1, slots), F32)
        statics = jnp.concatenate([fr, q, qd, sc, lb, jnp.zeros((1, slots), F32)], axis=0)
        send[...] = jnp.broadcast_to(statics[None], (devices, 8, slots))
        ones = jnp.ones((8, LANES), BF16)
        for k, unit in enumerate(UNITS):
            hit = slot_col == repeated[k : k + 1]
            picked = row_dot(values, hit.astype(F32))
            row = jnp.sum(jnp.where(wanted, picked, 0.0), axis=0, keepdims=True)
            row = jnp.where(first, repeated[k : k + 1], row)
            side = (k % 2) * LANES
            send[linear(cell, unit, sizes), 7:8, side : side + LANES] = row
            departed = departed + lax.dot_general(
                ones,
                hit.astype(F32).astype(BF16),
                (((1,), (1,)), ((), ())),
                preferred_element_type=F32,
            )[0:1]
        alive = live.astype(F32)
        gain = jnp.where(live, DRUDE_GAIN * qd, 0.0)
        own[...] = jnp.concatenate(
            [fr, q, qd, sc, lb, ms, ve, alive, jnp.where(departed > 0.5, 0.0, alive)]
            + [MOMENT * (gain * qd), gain, KICK * q / ms],
            axis=0,
        )

    return kernel


def columns(rows):
    lanes = rows.shape[1]
    padded = jnp.concatenate([rows, jnp.zeros((LANES - rows.shape[0], lanes), F32)], axis=0)
    return padded.T


def derived(fr, qd, sc, length):
    root = (DRUDE_GAIN**-0.5) / jnp.abs(qd)
    return fr * length, root, (0.25 * CUTOFF**3) * sc * root


def target_of(block, length, count):
    rows = block.shape[0]
    wide = [jnp.broadcast_to(block[:, c : c + 1], (rows, LANES)) for c in range(count)]
    shifted = [{-1: wide[a] + length, 0: wide[a], 1: wide[a] - length} for a in range(3)]
    return wide, shifted


def reader(source, place, half, rows):
    lanes = slice(half * LANES, (half + 1) * LANES)
    return lambda c: jnp.broadcast_to(source[place, c : c + 1, lanes], (rows, LANES))


def offsets(wide, shifted, row, box, length):
    deltas = []
    for a in range(3):
        step, nearest = box[a]
        if nearest:
            raw = wide[a] - row(a)
            deltas.append(raw - jnp.where(raw > 0.0, length, -length))
        else:
            deltas.append(shifted[a][step] - row(a))
    return deltas


def norm(deltas):
    return deltas[0] * deltas[0] + deltas[1] * deltas[1] + deltas[2] * deltas[2]


def terms(wide, dist_sq, row):
    inverse = lax.rsqrt(dist_sq)
    fade = inverse * jnp.maximum(1.0 - dist_sq, 0.0)
    half_x = (wide[3] * row(5) + wide[4] * row(4)) * (dist_sq * (dist_sq * inverse))
    tanh = jnp.tanh(half_x)
    root = lax.rsqrt(1.0 + tanh)
    base = ((fade * fade) * inverse) * (root * root)
    return inverse, half_x, tanh, base


def charge_sum(fields, wide, deltas, direct, row):
    weight = jnp.where(wide[5] != row(6), direct, 0.0) * row(3)
    return [fields[a] + weight * deltas[a] for a in range(3)]


def image_list(boxes):
    first, rest = [], []
    for n, box in enumerate(boxes):
        combos = list(itertools.product(*[(1, -1) if nearest else (step,) for step, nearest in box]))
        first.append((n, combos[0]))
        rest.extend((n, combo) for combo in combos[1:])
    return first + rest


def is_center(box):
    return all(step == 0 for step, _ in box)


def rows_of(parts):
    return [jnp.sum(part.T, axis=0, keepdims=True) for part in parts]


def send_moments(send, moments, slots):
    rows = [m[:, h * LANES : (h + 1) * LANES] for m in moments for h in range(slots // LANES)]
    rows.append(jnp.zeros((send.shape[1] - len(rows), LANES), F32))
    block = jnp.concatenate(rows, axis=0)
    send[...] = jnp.broadcast_to(block[None], send.shape)


def split(values):
    high = values.astype(BF16)
    return high, (values - high.astype(F32)).astype(BF16)


def field_kernel(sizes, slots, tile):
    boxes = shell(sizes)
    images = image_list(boxes)
    length = box_length(slots) / CUTOFF

    def kernel(recv, own, source, frames, ahi, alo, bhi, blo, perm, send, chosen, cols, acc):
        fr, root, part = derived(recv[:, 0:3, :], recv[:, 4:5, :], recv[:, 5:6, :], length)
        source[:, 0:3, :] = fr
        source[:, 3:4, :] = (2.0 / CUTOFF**2) * recv[:, 3:4, :]
        source[:, 4:5, :] = root
        source[:, 5:6, :] = part
        source[:, 6:8, :] = recv[:, 6:8, :]
        places = around(own_cell(), CENTERS[0], boxes, sizes)
        for n in range(len(boxes)):
            chosen[n] = source[places[n]]
        for n in range(len(boxes), chosen.shape[0]):
            chosen[n] = jnp.zeros((8, slots), F32)
        group = LANES // 8
        for g in range(chosen.shape[0] // group):
            cols[:, g * LANES : (g + 1) * LANES] = chosen[g * group : (g + 1) * group].reshape(LANES, slots).T
        one = jnp.ones((1, slots), F32)
        for m, (n, step) in enumerate(images):
            spots = [chosen[n, a : a + 1, :] + (step[a] - 0.5) * length for a in range(3)]
            frames[m] = jnp.concatenate(spots + [one] + spots + [one], axis=0)
        fr, root, part = derived(own[0:3], own[4:5], own[5:6], length)
        wide = [jnp.broadcast_to(row, (tile, slots)) for row in (fr[0:1], fr[1:2], fr[2:3], root, part, own[6:7])]
        acc[...] = jnp.zeros(acc.shape, F32)

        def body(t, carry):
            at = pl.ds(pl.multiple_of(t * tile, tile), tile)
            block = cols[at, :]
            fields = [acc[a] for a in range(3)]
            for n, box in enumerate(boxes):
                row = lambda c: jnp.broadcast_to(block[:, n * 8 + c : n * 8 + c + 1], (tile, slots))
                deltas, ahead = [], []
                for a in range(3):
                    step, nearest = box[a]
                    raw = wide[a] - row(a) if nearest or not step else (wide[a] - step * length) - row(a)
                    if nearest:
                        ahead.append((a, raw > 0.0))
                        raw = raw - jnp.where(ahead[-1][1], length, -length)
                    deltas.append(raw)
                dist_sq = norm(deltas)
                if is_center(box):
                    target = lax.broadcasted_iota(jnp.int32, (tile, slots), 1)
                    keep = target != lax.broadcasted_iota(jnp.int32, (tile, slots), 0) + t * tile
                    dist_sq = jnp.where(keep, dist_sq, 1.0)
                inverse, half_x, tanh, base = terms(wide, dist_sq, row)
                direct = base * tanh
                fields = charge_sum(fields, wide, deltas, direct, row)
                radial = (base * (3.0 * inverse)) * (inverse * (tanh - half_x * (1.0 - tanh)))
                if is_center(box):
                    direct = jnp.where(keep, direct, 0.0)
                    radial = jnp.where(keep, radial, 0.0)
                spot = pl.ds(pl.multiple_of(n * slots + t * tile, tile), tile)
                bhi[spot, :], blo[spot, :] = split(direct)
                for m, (owner, step) in enumerate(images):
                    if owner != n:
                        continue
                    part = radial
                    for a, side in ahead:
                        part = jnp.where(side, part, 0.0) if step[a] > 0 else jnp.where(side, 0.0, part)
                    spot = pl.ds(pl.multiple_of(m * slots + t * tile, tile), tile)
                    ahi[spot, :], alo[spot, :] = split(part)
            for a in range(3):
                acc[a] = fields[a]
            return carry

        lax.fori_loop(0, slots // tile, body, 0)
        rows = [jnp.sum(acc[a], axis=0, keepdims=True) for a in range(3)]
        perm[...] = jnp.concatenate(rows, axis=0)
        send_moments(send, [own[13:14] * row for row in rows], slots)

    return kernel


def build_lhs(lhs, recv, frames, places, images, slots):
    halves = slots // LANES
    upper = lax.broadcasted_iota(jnp.int32, (8, slots), 0) < 4
    known = {}
    for m, (n, _) in enumerate(images):
        if n not in known:
            known[n] = [
                jnp.concatenate(
                    [recv[places[n], a * halves + h : a * halves + h + 1, :] for h in range(halves)], axis=1
                )
                for a in range(3)
            ]
        mu = known[n]
        along = frames[m, 0:1, :] * mu[0] + frames[m, 1:2, :] * mu[1] + frames[m, 2:3, :] * mu[2]
        frame = frames[m]
        whole = lambda row: jnp.broadcast_to(row, (8, slots))
        value = jnp.concatenate(
            [
                frame * jnp.where(upper, whole(mu[0]), whole(mu[1])),
                frame * jnp.where(upper, whole(mu[2]), whole(along)),
            ],
            axis=0,
        )
        lanes = slice(m * slots, (m + 1) * slots)
        for piece in range(3):
            high = value.astype(BF16)
            lhs[piece * 16 : (piece + 1) * 16, lanes] = high
            value = value - high.astype(F32)


def induced_rows(lhs, ahi, alo, bhi, blo, own, perm, count_boxes, slots):
    length = box_length(slots) / CUTOFF
    dot = lambda left, right: jnp.dot(left, right, preferred_element_type=F32)
    near = lhs[:, 0 : count_boxes * slots]
    tensor = dot(lhs[...], ahi[...]) + dot(lhs[...], alo[...])
    plain = dot(near, bhi[...]) + dot(near, blo[...])
    tensor = tensor[0:16] + (tensor[16:32] + tensor[32:48])
    plain = plain[0:16] + (plain[16:32] + plain[32:48])
    spot = [(own[a : a + 1] - 0.5) * length for a in range(3)]
    first = [tensor[4 * a + 3 : 4 * a + 4] for a in range(3)]
    along = spot[0] * first[0] + spot[1] * first[1] + spot[2] * first[2] - tensor[15:16]
    rows = []
    for a in range(3):
        mixed = sum(tensor[4 * b + a : 4 * b + a + 1] * spot[b] for b in range(3))
        value = (spot[a] * along - mixed) + tensor[12 + a : 13 + a]
        rows.append(perm[a : a + 1] + (value - plain[4 * a + 3 : 4 * a + 4]))
    return rows


def induced_kernel(sizes, slots):
    boxes = shell(sizes)
    images = image_list(boxes)

    def kernel(recv, frames, ahi, alo, bhi, blo, own, perm, send, shift, lhs):
        places = around(own_cell(), CENTERS[0], boxes, sizes)
        build_lhs(lhs, recv, frames, places, images, slots)
        rows = induced_rows(lhs, ahi, alo, bhi, blo, own, perm, len(boxes), slots)
        shift[...] = jnp.concatenate([own[14:15] * row for row in rows], axis=0)
        send_moments(send, [own[13:14] * row for row in rows], slots)

    return kernel


def final_kernel(sizes, slots, moves):
    boxes = shell(sizes)
    images = image_list(boxes)
    tile = moves
    halves = slots // LANES
    edge = box_length(slots)
    length = edge / CUTOFF

    def kernel(
        recv, frames, ahi, alo, bhi, blo, own, perm, shift, first_recv, source,
        staying, arrivals, lhs, acc, cols, table, out_stay, out_come, out_sems,
    ):
        cell = own_cell()
        places = around(cell, CENTERS[0], boxes, sizes)
        build_lhs(lhs, recv, frames, places, images, slots)
        field = induced_rows(lhs, ahi, alo, bhi, blo, own, perm, len(boxes), slots)
        remain = own[12:13] > 0.5
        fast = [own[8 + a : 9 + a] + own[15:16] * field[a] for a in range(3)]
        place = [own[a : a + 1] + TIMESTEP * fast[a] / edge for a in range(3)]
        drude = [shift[a : a + 1] for a in range(3)]
        for r, row in enumerate(place + fast + drude):
            out_stay[r] = jnp.where(remain, row, 0.0)
        early = pltpu.make_async_copy(out_stay, staying, out_sems.at[0])
        early.start()

        fill_table(table, cell, boxes, sizes)
        lane = lax.broadcasted_iota(jnp.int32, (1, LANES), 1)
        origin = [linear(cell, [-step for step in unit], sizes) for unit in UNITS]
        extra = jnp.full((8, LANES), -1.0, F32)
        for k in range(6):
            side = (k % 2) * LANES
            row = first_recv[origin[k], 7:8, side : side + LANES]
            row = jnp.broadcast_to(row, (8, LANES))
            fields = [pltpu.roll(row, (k * moves - c * moves) % LANES, 1)[0:1] for c in range(5)]
            block = jnp.concatenate(fields + [extra[0:3]], axis=0)
            extra = jnp.where(lane // moves == k, block, extra)
        slot = extra[0:1]
        slot_col = lax.broadcasted_iota(jnp.int32, (slots, LANES), 0).astype(F32)
        hit = (slot_col == slot).astype(F32)
        got = jnp.zeros((8, LANES), F32)
        moment = jnp.zeros((8, LANES), F32)
        for k in range(6):
            got = jnp.where(lane // moves == k, row_dot(first_recv[origin[k]], hit), got)
            block = recv[origin[k]]
            both = [row_dot(block, hit[h * LANES : (h + 1) * LANES, :]) for h in range(halves)]
            one = [
                sum(both[h][a * halves + h : a * halves + h + 1] for h in range(halves)) for a in range(3)
            ]
            one = jnp.concatenate(one + [jnp.zeros((5, LANES), F32)], axis=0)
            moment = jnp.where(lane // moves == k, one, moment)
        present = slot >= 0.0
        fr, root, part = derived(got[0:3], jnp.where(present, got[4:5], -1.0), got[5:6], length)
        cols[...] = columns(jnp.concatenate([fr, root, part, got[6:7], slot, slot], axis=0))
        acc[...] = jnp.zeros(acc.shape, F32)

        def incoming(k, carry):
            at = pl.ds(pl.multiple_of(k * tile, tile), tile)
            wide, shifted = target_of(cols[at, :], length, 7)
            fields = [jnp.zeros((tile, LANES), F32)] * 3
            for n, box in enumerate(boxes):
                spot = table[(k + 1) * len(boxes) + n]
                for half in range(halves):
                    row = reader(source, spot, half, tile)
                    mu = [
                        jnp.broadcast_to(recv[spot, a * halves + half : a * halves + half + 1, :], (tile, LANES))
                        for a in range(3)
                    ]
                    deltas = offsets(wide, shifted, row, box, length)
                    dist_sq = norm(deltas)
                    if is_center(box):
                        ids = lax.broadcasted_iota(jnp.int32, (tile, LANES), 1) + half * LANES
                        keep = wide[6] != ids.astype(F32)
                        dist_sq = jnp.where(keep, dist_sq, 1.0)
                    inverse, half_x, tanh, base = terms(wide, dist_sq, row)
                    direct = base * tanh
                    radial = (base * (3.0 * inverse)) * (inverse * (tanh - half_x * (1.0 - tanh)))
                    if is_center(box):
                        direct = jnp.where(keep, direct, 0.0)
                        radial = jnp.where(keep, radial, 0.0)
                    pull = jnp.where(wide[5] != row(6), direct, 0.0) * row(3)
                    pull = pull + radial * (deltas[0] * mu[0] + deltas[1] * mu[1] + deltas[2] * mu[2])
                    fields = [fields[a] + (pull * deltas[a] - direct * mu[a]) for a in range(3)]
            for a in range(3):
                acc[a, at, :] = fields[a]
            return carry

        lax.fori_loop(0, 6, incoming, 0)
        pull = rows_of([acc[a] for a in range(3)])
        q = got[3:4]
        qd = got[4:5]
        mass = jnp.where(present, extra[4:5], 1.0)
        gain = KICK * q / mass
        fast = [extra[1 + a : 2 + a] + gain * pull[a] for a in range(3)]
        place = [got[a : a + 1] + TIMESTEP * fast[a] / edge for a in range(3)]
        for k, unit in enumerate(UNITS):
            for a in range(3):
                if unit[a]:
                    place[a] = place[a] - jnp.where(lane // moves == k, float(unit[a]), 0.0)
        safe = jnp.where(present, qd, -1.0) * MOMENT
        drude = [moment[a : a + 1] / safe for a in range(3)]
        record = place + fast + drude + [q, qd, got[5:6], got[6:7], mass]
        for r, row in enumerate(record):
            out_come[r] = jnp.where(present, row, 0.0)[:, 0 : 6 * moves]
        late = pltpu.make_async_copy(out_come, arrivals, out_sems.at[1])
        late.start()
        early.wait()
        late.wait()

    return kernel


def solution(mesh):
    sizes = tuple(mesh.shape[axis] for axis in AXES)
    devices = int(np.prod(sizes))
    boxes = shell(sizes)
    count_boxes = len(boxes)
    count_images = len(image_list(boxes))
    padded_boxes = -(-count_boxes // 16) * 16

    def local(fractions, velocity, charge, drude_charge, screening, labels, masses, counts, leaving):
        slots = charge.shape[-1]
        moves = leaving.shape[-1]
        exchange = lambda block: lax.all_to_all(block, AXES, 0, 0)
        shape = lambda *dims: jax.ShapeDtypeStruct(dims, F32)
        half = lambda *dims: jax.ShapeDtypeStruct(dims, BF16)
        hbm = lambda x: pltpu.with_memory_space_constraint(x, pltpu.HBM)
        moment_shape = (devices, 8, LANES)
        dma = pltpu.SemaphoreType.DMA

        def call(kernel, in_specs, outs, out_specs, scratch, flops, limit):
            return pl.pallas_call(
                kernel,
                in_specs=in_specs,
                out_shape=outs,
                out_specs=out_specs,
                scratch_shapes=scratch,
                compiler_params=pltpu.CompilerParams(vmem_limit_bytes=limit),
                cost_estimate=pl.CostEstimate(flops=flops, bytes_accessed=1 << 20, transcendentals=0),
            )

        flat = [
            fractions.reshape(3, 1, slots),
            velocity.reshape(3, 1, slots),
            charge.reshape(1, slots),
            drude_charge.reshape(1, slots),
            screening.reshape(1, slots),
            labels.reshape(1, slots),
            masses.reshape(1, slots),
            leaving.reshape(6, 1, moves),
        ]
        send, own = call(
            pack_kernel(sizes, slots, moves),
            [smem()] + [anywhere()] * 8,
            (shape(devices, 8, slots), shape(16, slots)),
            (vmem(), vmem()),
            [VMEM(array.shape, array.dtype) for array in flat] + [dma((8,))],
            1 << 20,
            8 << 20,
        )(counts.reshape(1), *[hbm(x) for x in flat])
        first = exchange(send)
        outs = (
            shape(devices, 8, slots),
            shape(count_images, 8, slots),
            half(count_images * slots, slots),
            half(count_images * slots, slots),
            half(count_boxes * slots, slots),
            half(count_boxes * slots, slots),
            shape(3, slots),
            shape(*moment_shape),
        )
        source, frames, ahi, alo, bhi, blo, perm, moments = call(
            field_kernel(sizes, slots, 16),
            [vmem()] * 2,
            outs,
            (vmem(),) * len(outs),
            [
                VMEM((padded_boxes, 8, slots), F32),
                VMEM((slots, padded_boxes * 8), F32),
                VMEM((3, 16, slots), F32),
            ],
            1 << 25,
            8 << 20,
        )(first, own)
        got = exchange(moments)
        tensors = (frames, ahi, alo, bhi, blo, own, perm)
        lhs = VMEM((48, count_images * slots), BF16)
        for _ in range(ITERS - 1):
            moments, shift = call(
                induced_kernel(sizes, slots),
                [vmem()] * 8,
                (shape(*moment_shape), shape(3, slots)),
                (vmem(),) * 2,
                [lhs],
                1 << 24,
                4 << 20,
            )(got, *tensors)
            got = exchange(moments)
        staying, arrivals = call(
            final_kernel(sizes, slots, moves),
            [vmem()] * 11,
            (pltpu.HBM((9, 1, slots), F32), pltpu.HBM((14, 1, 6 * moves), F32)),
            (anywhere(), anywhere()),
            [
                lhs,
                VMEM((3, LANES, LANES), F32),
                VMEM((LANES, LANES), F32),
                pltpu.SMEM((len(CENTERS) * count_boxes,), jnp.int32),
                VMEM((9, 1, slots), F32),
                VMEM((14, 1, 6 * moves), F32),
                dma((2,)),
            ],
            1 << 24,
            8 << 20,
        )(got, *tensors, shift, first, source)
        return staying.reshape(1, 1, 1, 9, slots), arrivals.reshape(1, 1, 1, 14, 6 * moves)

    box = P("gx", "gy", "gz", None)
    rows = P("gx", "gy", "gz", None, None)
    return jax.shard_map(
        local,
        mesh=mesh,
        in_specs=(rows, rows, box, box, box, box, box, P("gx", "gy", "gz"), rows),
        out_specs=(rows, rows),
        check_vma=False,
    )
```

```python
import itertools

import jax
import jax.numpy as jnp
import numpy as np
from jax import lax
from jax.experimental import pallas as pl
from jax.experimental.pallas import tpu as pltpu
from jax.sharding import PartitionSpec as P

ITERS = 3
CUTOFF = 12.0
DRUDE_GAIN = 0.3320636
KICK = 0.002 * 418.4 * 332.0636
TIMESTEP = 0.002
UNITS = ((1, 0, 0), (-1, 0, 0), (0, 1, 0), (0, -1, 0), (0, 0, 1), (0, 0, -1))
AXES = ("gx", "gy", "gz")
LANES = 128
CENTERS = ((0, 0, 0),) + tuple(tuple(-step for step in unit) for unit in UNITS)
MOMENT = 2.0 / CUTOFF**3
F32 = jnp.float32
BF16 = jnp.bfloat16
VMEM = pltpu.VMEM


def vmem():
    return pl.BlockSpec(memory_space=pltpu.VMEM)


def smem():
    return pl.BlockSpec(memory_space=pltpu.SMEM)


def anywhere():
    return pl.BlockSpec(memory_space=pltpu.HBM)


def box_length(slots):
    return max(12.0, (10.0 * slots) ** (1.0 / 3.0))


def axis_steps(count):
    return ((0, False), (1, True)) if count == 2 else ((-1, False), (0, False), (1, False))


def shell(sizes):
    return list(itertools.product(*[axis_steps(count) for count in sizes]))


def own_cell():
    return [lax.axis_index(axis) for axis in AXES]


def linear(cell, steps, sizes):
    value = 0
    for coordinate, step, count in zip(cell, steps, sizes):
        value = value * count + (coordinate + (step % count)) % count
    return value


def around(cell, center, boxes, sizes):
    return [linear(cell, [center[a] + box[a][0] for a in range(3)], sizes) for box in boxes]


def fill_table(table, cell, boxes, sizes):
    for g, center in enumerate(CENTERS):
        for n, place in enumerate(around(cell, center, boxes, sizes)):
            table[g * len(boxes) + n] = place


def pieces_of(values):
    pieces = []
    for _ in range(3):
        piece = values.astype(BF16).astype(F32)
        pieces.append(piece)
        values = values - piece
    return pieces


def pick(blocks, hit):
    count = blocks.shape[0]
    stacked = jnp.concatenate(pieces_of(blocks), axis=0).astype(BF16)
    got = jnp.dot(stacked, hit, preferred_element_type=F32)
    return (got[0:count] + got[count : 2 * count]) + got[2 * count :]


def pack_kernel(sizes, slots, moves):
    devices = int(np.prod(sizes))

    def kernel(*refs):
        count, inputs, (send, own), staged, sems = refs[0], refs[1:9], refs[9:11], refs[11:19], refs[19]
        copies = [pltpu.make_async_copy(inputs[i], staged[i], sems.at[i]) for i in range(8)]
        for copy in copies:
            copy.start()
        for copy in copies:
            copy.wait()
        frac, vel, charge, drude, screen, label, mass, leaving = staged
        cell = own_cell()
        lane = lax.broadcasted_iota(jnp.int32, (1, slots), 1)
        live = lane < count[0]
        fr = jnp.concatenate([frac[a] for a in range(3)], axis=0)
        ve = jnp.concatenate([vel[a] for a in range(3)], axis=0)
        q = jnp.where(live, charge[...], 0.0)
        qd = jnp.where(live, drude[...], -1.0)
        sc = screen[...]
        lb = label[...].astype(F32)
        ms = mass[...]
        lv = jnp.concatenate([leaving[k].astype(F32) for k in range(6)], axis=0)
        lv = jnp.concatenate([lv, jnp.full((2, moves), -1.0, F32)], axis=0)
        spread = (
            lax.broadcasted_iota(jnp.int32, (moves, LANES), 1) % moves
            == lax.broadcasted_iota(jnp.int32, (moves, LANES), 0)
        ).astype(F32)
        repeated = jnp.dot(lv.astype(BF16), spread.astype(BF16), preferred_element_type=F32)
        slot_col = lax.broadcasted_iota(jnp.int32, (slots, LANES), 0).astype(F32)
        values = jnp.concatenate([ve, ms, jnp.zeros((4, slots), F32)], axis=0)
        field = lax.broadcasted_iota(jnp.int32, (8, LANES), 1) // moves - 1
        wanted = field == lax.broadcasted_iota(jnp.int32, (8, LANES), 0)
        first = lax.broadcasted_iota(jnp.int32, (1, LANES), 1) < moves
        statics = jnp.concatenate([fr, q, qd, sc, lb, jnp.zeros((1, slots), F32)], axis=0)
        send[...] = jnp.broadcast_to(statics[None], (devices, 8, slots))
        hits = jnp.concatenate(
            [(slot_col == repeated[k : k + 1]).astype(F32).astype(BF16) for k in range(6)], axis=1
        )
        picked = pick(values, hits)
        for k, unit in enumerate(UNITS):
            mine = picked[:, k * LANES : (k + 1) * LANES]
            row = jnp.sum(jnp.where(wanted, mine, 0.0), axis=0, keepdims=True)
            row = jnp.where(first, repeated[k : k + 1], row)
            side = (k % 2) * LANES
            send[linear(cell, unit, sizes), 7:8, side : side + LANES] = row
        ones = jnp.ones((16, 6 * LANES), BF16)
        departed = lax.dot_general(ones, hits, (((1,), (1,)), ((), ())), preferred_element_type=F32)[0:1]
        alive = live.astype(F32)
        gain = jnp.where(live, DRUDE_GAIN * qd, 0.0)
        own[...] = jnp.concatenate(
            [fr, q, qd, sc, lb, ms, ve, alive, jnp.where(departed > 0.5, 0.0, alive)]
            + [MOMENT * (gain * qd), gain, KICK * q / ms],
            axis=0,
        )

    return kernel


def columns(rows):
    lanes = rows.shape[1]
    padded = jnp.concatenate([rows, jnp.zeros((LANES - rows.shape[0], lanes), F32)], axis=0)
    return padded.T


def derived(fr, qd, sc, length):
    root = (DRUDE_GAIN**-0.5) / jnp.abs(qd)
    return fr * length, root, (0.25 * CUTOFF**3) * sc * root


def target_of(block, length, count):
    rows = block.shape[0]
    wide = [jnp.broadcast_to(block[:, c : c + 1], (rows, LANES)) for c in range(count)]
    shifted = [{-1: wide[a] + length, 0: wide[a], 1: wide[a] - length} for a in range(3)]
    return wide, shifted


def reader(source, place, half, rows):
    lanes = slice(half * LANES, (half + 1) * LANES)
    return lambda c: jnp.broadcast_to(source[place, c : c + 1, lanes], (rows, LANES))


def offsets(wide, shifted, row, box, length):
    deltas = []
    for a in range(3):
        step, nearest = box[a]
        if nearest:
            raw = wide[a] - row(a)
            deltas.append(raw - jnp.where(raw > 0.0, length, -length))
        else:
            deltas.append(shifted[a][step] - row(a))
    return deltas


def norm(deltas):
    return deltas[0] * deltas[0] + deltas[1] * deltas[1] + deltas[2] * deltas[2]


def terms(wide, dist_sq, row):
    inverse = lax.rsqrt(dist_sq)
    fade = inverse * jnp.maximum(1.0 - dist_sq, 0.0)
    half_x = (wide[3] * row(5) + wide[4] * row(4)) * (dist_sq * (dist_sq * inverse))
    tanh = jnp.tanh(half_x)
    root = fade * lax.rsqrt(1.0 + tanh)
    base = (root * root) * inverse
    return inverse, half_x, tanh, base


def charge_sum(fields, wide, deltas, direct, row):
    weight = jnp.where(wide[5] != row(6), direct, 0.0) * row(3)
    return [fields[a] + weight * deltas[a] for a in range(3)]


def image_list(boxes):
    first, rest = [], []
    for n, box in enumerate(boxes):
        combos = list(itertools.product(*[(1, -1) if nearest else (step,) for step, nearest in box]))
        first.append((n, combos[0]))
        rest.extend((n, combo) for combo in combos[1:])
    return first + rest


def is_center(box):
    return all(step == 0 for step, _ in box)


def rows_of(parts):
    return [jnp.sum(part.T, axis=0, keepdims=True) for part in parts]


def send_moments(send, moments, slots):
    halves = slots // LANES
    for a in range(3):
        for h in range(halves):
            row = moments[a][:, h * LANES : (h + 1) * LANES]
            send[:, a * halves + h] = jnp.broadcast_to(row[None], (send.shape[0], 1, LANES))


def split(values):
    high = values.astype(BF16)
    return high, (values - high.astype(F32)).astype(BF16)


def field_kernel(sizes, slots, tile):
    boxes = shell(sizes)
    images = image_list(boxes)
    length = box_length(slots) / CUTOFF

    def kernel(recv, own, source, frames, ahi, alo, bhi, blo, perm, send, chosen, cols, acc):
        fr, root, part = derived(recv[:, 0:3, :], recv[:, 4:5, :], recv[:, 5:6, :], length)
        source[:, 0:3, :] = fr
        source[:, 3:4, :] = (2.0 / CUTOFF**2) * recv[:, 3:4, :]
        source[:, 4:5, :] = root
        source[:, 5:6, :] = part
        source[:, 6:8, :] = recv[:, 6:8, :]
        places = around(own_cell(), CENTERS[0], boxes, sizes)
        for n in range(len(boxes)):
            chosen[n] = source[places[n]]
        for n in range(len(boxes), chosen.shape[0]):
            chosen[n] = jnp.zeros((8, slots), F32)
        group = LANES // 8
        for g in range(chosen.shape[0] // group):
            cols[:, g * LANES : (g + 1) * LANES] = chosen[g * group : (g + 1) * group].reshape(LANES, slots).T
        one = jnp.ones((1, slots), F32)
        for m, (n, step) in enumerate(images):
            spots = [chosen[n, a : a + 1, :] + (step[a] - 0.5) * length for a in range(3)]
            frames[m] = jnp.concatenate(spots + [one] + spots + [one], axis=0)
        fr, root, part = derived(own[0:3], own[4:5], own[5:6], length)
        wide = [jnp.broadcast_to(row, (tile, slots)) for row in (fr[0:1], fr[1:2], fr[2:3], root, part, own[6:7])]
        acc[...] = jnp.zeros(acc.shape, F32)

        def body(t, carry):
            at = pl.ds(pl.multiple_of(t * tile, tile), tile)
            block = cols[at, :]
            fields = [acc[a] for a in range(3)]
            for n, box in enumerate(boxes):
                row = lambda c: jnp.broadcast_to(block[:, n * 8 + c : n * 8 + c + 1], (tile, slots))
                deltas, ahead = [], []
                for a in range(3):
                    step, nearest = box[a]
                    raw = wide[a] - row(a) if nearest or not step else (wide[a] - step * length) - row(a)
                    if nearest:
                        ahead.append((a, raw > 0.0))
                        raw = raw - jnp.where(ahead[-1][1], length, -length)
                    deltas.append(raw)
                dist_sq = norm(deltas)
                if is_center(box):
                    target = lax.broadcasted_iota(jnp.int32, (tile, slots), 1)
                    keep = target != lax.broadcasted_iota(jnp.int32, (tile, slots), 0) + t * tile
                    dist_sq = jnp.where(keep, dist_sq, 1.0)
                inverse, half_x, tanh, base = terms(wide, dist_sq, row)
                direct = base * tanh
                fields = charge_sum(fields, wide, deltas, direct, row)
                radial = base * (inverse * inverse) * (tanh - half_x * (1.0 - tanh))
                if is_center(box):
                    direct = jnp.where(keep, direct, 0.0)
                    radial = jnp.where(keep, radial, 0.0)
                spot = pl.ds(pl.multiple_of(n * slots + t * tile, tile), tile)
                bhi[spot, :], blo[spot, :] = split(direct)
                for m, (owner, step) in enumerate(images):
                    if owner != n:
                        continue
                    part = radial
                    for a, side in ahead:
                        part = jnp.where(side, part, 0.0) if step[a] > 0 else jnp.where(side, 0.0, part)
                    spot = pl.ds(pl.multiple_of(m * slots + t * tile, tile), tile)
                    ahi[spot, :], alo[spot, :] = split(part)
            for a in range(3):
                acc[a] = fields[a]
            return carry

        lax.fori_loop(0, slots // tile, body, 0)
        rows = [jnp.sum(acc[a], axis=0, keepdims=True) for a in range(3)]
        perm[...] = jnp.concatenate(rows, axis=0)
        send_moments(send, [own[13:14] * row for row in rows], slots)

    return kernel


def build_lhs(lhs, recv, frames, places, images, slots):
    halves = slots // LANES
    upper = lax.broadcasted_iota(jnp.int32, (8, slots), 0) < 4
    known = {}
    for m, (n, _) in enumerate(images):
        if n not in known:
            known[n] = [
                jnp.concatenate(
                    [recv[places[n], a * halves + h] for h in range(halves)], axis=1
                )
                for a in range(3)
            ]
        mu = known[n]
        along = frames[m, 0:1, :] * mu[0] + frames[m, 1:2, :] * mu[1] + frames[m, 2:3, :] * mu[2]
        frame = frames[m]
        whole = lambda row: jnp.broadcast_to(row, (8, slots))
        value = jnp.concatenate(
            [
                frame * jnp.where(upper, whole(mu[0]), whole(mu[1])),
                frame * jnp.where(upper, whole(mu[2]), whole(along)),
            ],
            axis=0,
        )
        lanes = slice(m * slots, (m + 1) * slots)
        for piece in range(3):
            high = value.astype(BF16)
            lhs[piece * 16 : (piece + 1) * 16, lanes] = high
            value = value - high.astype(F32)


def product(lhs, high, low, at):
    left = lhs[:, at]
    dot = lambda right: jnp.dot(left, right[at, :], preferred_element_type=F32)
    return dot(high) + dot(low)


def induced_rows(tensor, plain, own, perm, slots):
    length = box_length(slots) / CUTOFF
    tensor = 3.0 * (tensor[0:16] + (tensor[16:32] + tensor[32:48]))
    plain = plain[0:16] + (plain[16:32] + plain[32:48])
    spot = [(own[a : a + 1] - 0.5) * length for a in range(3)]
    first = [tensor[4 * a + 3 : 4 * a + 4] for a in range(3)]
    along = spot[0] * first[0] + spot[1] * first[1] + spot[2] * first[2] - tensor[15:16]
    rows = []
    for a in range(3):
        mixed = sum(tensor[4 * b + a : 4 * b + a + 1] * spot[b] for b in range(3))
        value = (spot[a] * along - mixed) + tensor[12 + a : 13 + a]
        rows.append(perm[a : a + 1] + (value - plain[4 * a + 3 : 4 * a + 4]))
    return rows


def induced_kernel(sizes, slots):
    boxes = shell(sizes)
    images = image_list(boxes)

    def kernel(recv, frames, ahi, alo, bhi, blo, own, perm, send, shift, lhs):
        places = around(own_cell(), CENTERS[0], boxes, sizes)
        build_lhs(lhs, recv, frames, places, images, slots)
        tensor = product(lhs, ahi, alo, slice(0, len(images) * slots))
        plain = product(lhs, bhi, blo, slice(0, len(boxes) * slots))
        rows = induced_rows(tensor, plain, own, perm, slots)
        shift[...] = jnp.concatenate([own[14:15] * row for row in rows], axis=0)
        send_moments(send, [own[13:14] * row for row in rows], slots)

    return kernel


def final_kernel(sizes, slots, moves):
    boxes = shell(sizes)
    images = image_list(boxes)
    tile = moves
    halves = slots // LANES
    edge = box_length(slots)
    length = edge / CUTOFF

    def kernel(
        recv, frames, ahi, alo, bhi, blo, own, perm, shift, first_recv, source,
        staying, arrivals, lhs, sums, acc, targets, table, out_stay, out_come, out_sems,
    ):
        cell = own_cell()
        places = around(cell, CENTERS[0], boxes, sizes)
        build_lhs(lhs, recv, frames, places, images, slots)
        fill_table(table, cell, boxes, sizes)
        lane = lax.broadcasted_iota(jnp.int32, (1, LANES), 1)
        origin = [linear(cell, [-step for step in unit], sizes) for unit in UNITS]
        extra = jnp.full((8, LANES), -1.0, F32)
        for k in range(6):
            side = (k % 2) * LANES
            row = first_recv[origin[k], 7:8, side : side + LANES]
            row = jnp.broadcast_to(row, (8, LANES))
            fields = [pltpu.roll(row, (k * moves - c * moves) % LANES, 1)[0:1] for c in range(5)]
            block = jnp.concatenate(fields + [extra[0:3]], axis=0)
            extra = jnp.where(lane // moves == k, block, extra)
        slot = extra[0:1]
        slot_col = lax.broadcasted_iota(jnp.int32, (slots, LANES), 0).astype(F32)
        hit = (slot_col == slot).astype(F32).astype(BF16)
        blank = jnp.zeros((5, slots), F32)
        blocks = []
        for k in range(6):
            blocks.append(first_recv[origin[k]])
            for a in range(3):
                blocks.append(
                    jnp.concatenate([recv[origin[k], a * halves + h] for h in range(halves)], axis=1)
                )
            blocks.append(blank)
        taken = pick(jnp.concatenate(blocks, axis=0), hit)
        got = jnp.zeros((8, LANES), F32)
        moment = jnp.zeros((8, LANES), F32)
        for k in range(6):
            got = jnp.where(lane // moves == k, taken[16 * k : 16 * k + 8], got)
            moment = jnp.where(lane // moves == k, taken[16 * k + 8 : 16 * k + 16], moment)
        present = slot >= 0.0
        fr, root, part = derived(got[0:3], jnp.where(present, got[4:5], -1.0), got[5:6], length)
        cols = columns(jnp.concatenate([fr, root, part, got[6:7], slot, slot], axis=0))
        for k in range(6):
            for c, value in enumerate(target_of(cols[k * tile : (k + 1) * tile], length, 7)[0]):
                targets[k, c] = value
        acc[...] = jnp.zeros(acc.shape, F32)
        steps = [len(images) // 6 * slots, len(boxes) // 6 * slots]
        for which, (high, low, count) in enumerate(((ahi, alo, len(images)), (bhi, blo, len(boxes)))):
            sums[which] = jnp.zeros((48, slots), F32)
            if count * slots > 6 * steps[which]:
                sums[which] = product(lhs, high, low, slice(6 * steps[which], count * slots))

        def incoming(k, carry):
            for which, (high, low) in enumerate(((ahi, alo), (bhi, blo))):
                part = pl.ds(pl.multiple_of(k * steps[which], LANES), steps[which])
                sums[which] = sums[which] + product(lhs, high, low, part)
            at = pl.ds(pl.multiple_of(k * tile, tile), tile)
            wide = [targets[k, c] for c in range(7)]
            shifted = [{-1: wide[a] + length, 0: wide[a], 1: wide[a] - length} for a in range(3)]
            fields = [jnp.zeros((tile, LANES), F32)] * 3
            for n, box in enumerate(boxes):
                spot = table[(k + 1) * len(boxes) + n]
                for half in range(halves):
                    row = reader(source, spot, half, tile)
                    mu = [
                        jnp.broadcast_to(recv[spot, a * halves + half], (tile, LANES))
                        for a in range(3)
                    ]
                    deltas = offsets(wide, shifted, row, box, length)
                    dist_sq = norm(deltas)
                    if is_center(box):
                        ids = lax.broadcasted_iota(jnp.int32, (tile, LANES), 1) + half * LANES
                        keep = wide[6] != ids.astype(F32)
                        dist_sq = jnp.where(keep, dist_sq, 1.0)
                    inverse, half_x, tanh, base = terms(wide, dist_sq, row)
                    direct = base * tanh
                    radial = base * (inverse * inverse) * (tanh - half_x * (1.0 - tanh))
                    if is_center(box):
                        direct = jnp.where(keep, direct, 0.0)
                        radial = jnp.where(keep, radial, 0.0)
                    pull = jnp.where(wide[5] != row(6), direct, 0.0) * row(3)
                    pull = pull + (3.0 * radial) * (deltas[0] * mu[0] + deltas[1] * mu[1] + deltas[2] * mu[2])
                    fields = [fields[a] + (pull * deltas[a] - direct * mu[a]) for a in range(3)]
            for a in range(3):
                acc[a, at, :] = fields[a]
            return carry

        lax.fori_loop(0, 6, incoming, 0)
        field = induced_rows(sums[0], sums[1], own, perm, slots)
        remain = own[12:13] > 0.5
        fast = [own[8 + a : 9 + a] + own[15:16] * field[a] for a in range(3)]
        place = [own[a : a + 1] + TIMESTEP * fast[a] / edge for a in range(3)]
        drude = [shift[a : a + 1] for a in range(3)]
        for r, row in enumerate(place + fast + drude):
            out_stay[r] = jnp.where(remain, row, 0.0)
        early = pltpu.make_async_copy(out_stay, staying, out_sems.at[0])
        early.start()

        pull = rows_of([acc[a] for a in range(3)])
        q = got[3:4]
        qd = got[4:5]
        mass = jnp.where(present, extra[4:5], 1.0)
        gain = KICK * q / mass
        fast = [extra[1 + a : 2 + a] + gain * pull[a] for a in range(3)]
        place = [got[a : a + 1] + TIMESTEP * fast[a] / edge for a in range(3)]
        for k, unit in enumerate(UNITS):
            for a in range(3):
                if unit[a]:
                    place[a] = place[a] - jnp.where(lane // moves == k, float(unit[a]), 0.0)
        safe = jnp.where(present, qd, -1.0) * MOMENT
        drude = [moment[a : a + 1] / safe for a in range(3)]
        record = place + fast + drude + [q, qd, got[5:6], got[6:7], mass]
        for r, row in enumerate(record):
            out_come[r] = jnp.where(present, row, 0.0)[:, 0 : 6 * moves]
        late = pltpu.make_async_copy(out_come, arrivals, out_sems.at[1])
        late.start()
        early.wait()
        late.wait()

    return kernel


def solution(mesh):
    sizes = tuple(mesh.shape[axis] for axis in AXES)
    devices = int(np.prod(sizes))
    boxes = shell(sizes)
    count_boxes = len(boxes)
    count_images = len(image_list(boxes))
    padded_boxes = -(-count_boxes // 16) * 16

    def local(fractions, velocity, charge, drude_charge, screening, labels, masses, counts, leaving):
        slots = charge.shape[-1]
        moves = leaving.shape[-1]
        exchange = lambda block: lax.all_to_all(block, AXES, 0, 0)
        shape = lambda *dims: jax.ShapeDtypeStruct(dims, F32)
        half = lambda *dims: jax.ShapeDtypeStruct(dims, BF16)
        hbm = lambda x: pltpu.with_memory_space_constraint(x, pltpu.HBM)
        moment_shape = (devices, 3 * (slots // LANES), 1, LANES)
        dma = pltpu.SemaphoreType.DMA

        def call(kernel, in_specs, outs, out_specs, scratch, flops, limit):
            return pl.pallas_call(
                kernel,
                in_specs=in_specs,
                out_shape=outs,
                out_specs=out_specs,
                scratch_shapes=scratch,
                compiler_params=pltpu.CompilerParams(vmem_limit_bytes=limit),
                cost_estimate=pl.CostEstimate(flops=flops, bytes_accessed=1 << 20, transcendentals=0),
            )

        flat = [
            fractions.reshape(3, 1, slots),
            velocity.reshape(3, 1, slots),
            charge.reshape(1, slots),
            drude_charge.reshape(1, slots),
            screening.reshape(1, slots),
            labels.reshape(1, slots),
            masses.reshape(1, slots),
            leaving.reshape(6, 1, moves),
        ]
        send, own = call(
            pack_kernel(sizes, slots, moves),
            [smem()] + [anywhere()] * 8,
            (shape(devices, 8, slots), shape(16, slots)),
            (vmem(), vmem()),
            [VMEM(array.shape, array.dtype) for array in flat] + [dma((8,))],
            1 << 20,
            8 << 20,
        )(counts.reshape(1), *[hbm(x) for x in flat])
        first = exchange(send)
        outs = (
            shape(devices, 8, slots),
            shape(count_images, 8, slots),
            half(count_images * slots, slots),
            half(count_images * slots, slots),
            half(count_boxes * slots, slots),
            half(count_boxes * slots, slots),
            shape(3, slots),
            shape(*moment_shape),
        )
        source, frames, ahi, alo, bhi, blo, perm, moments = call(
            field_kernel(sizes, slots, 32),
            [vmem()] * 2,
            outs,
            (vmem(),) * len(outs),
            [
                VMEM((padded_boxes, 8, slots), F32),
                VMEM((slots, padded_boxes * 8), F32),
                VMEM((3, 32, slots), F32),
            ],
            1 << 25,
            8 << 20,
        )(first, own)
        got = exchange(moments)
        tensors = (frames, ahi, alo, bhi, blo, own, perm)
        lhs = VMEM((48, count_images * slots), BF16)
        for _ in range(ITERS - 1):
            moments, shift = call(
                induced_kernel(sizes, slots),
                [vmem()] * 8,
                (shape(*moment_shape), shape(3, slots)),
                (vmem(),) * 2,
                [lhs],
                1 << 24,
                4 << 20,
            )(got, *tensors)
            got = exchange(moments)
        staying, arrivals = call(
            final_kernel(sizes, slots, moves),
            [vmem()] * 11,
            (pltpu.HBM((9, 1, slots), F32), pltpu.HBM((14, 1, 6 * moves), F32)),
            (anywhere(), anywhere()),
            [
                lhs,
                VMEM((2, 48, slots), F32),
                VMEM((3, LANES, LANES), F32),
                VMEM((6, 7, moves, LANES), F32),
                pltpu.SMEM((len(CENTERS) * count_boxes,), jnp.int32),
                VMEM((9, 1, slots), F32),
                VMEM((14, 1, 6 * moves), F32),
                dma((2,)),
            ],
            1 << 24,
            8 << 20,
        )(got, *tensors, shift, first, source)
        return staying.reshape(1, 1, 1, 9, slots), arrivals.reshape(1, 1, 1, 14, 6 * moves)

    box = P("gx", "gy", "gz", None)
    rows = P("gx", "gy", "gz", None, None)
    return jax.shard_map(
        local,
        mesh=mesh,
        in_specs=(rows, rows, box, box, box, box, box, P("gx", "gy", "gz"), rows),
        out_specs=(rows, rows),
        check_vma=False,
    )
```

```python
import itertools

import jax
import jax.numpy as jnp
import numpy as np
from jax import lax
from jax.experimental import pallas as pl
from jax.experimental.pallas import tpu as pltpu
from jax.sharding import PartitionSpec as P

ITERS = 3
CUTOFF = 12.0
DRUDE_GAIN = 0.3320636
KICK = 0.002 * 418.4 * 332.0636
TIMESTEP = 0.002
UNITS = ((1, 0, 0), (-1, 0, 0), (0, 1, 0), (0, -1, 0), (0, 0, 1), (0, 0, -1))
AXES = ("gx", "gy", "gz")
LANES = 128
CENTERS = ((0, 0, 0),) + tuple(tuple(-step for step in unit) for unit in UNITS)
MOMENT = 2.0 / CUTOFF**3
F32 = jnp.float32
BF16 = jnp.bfloat16
VMEM = pltpu.VMEM


def vmem():
    return pl.BlockSpec(memory_space=pltpu.VMEM)


def smem():
    return pl.BlockSpec(memory_space=pltpu.SMEM)


def anywhere():
    return pl.BlockSpec(memory_space=pltpu.HBM)


def box_length(slots):
    return max(12.0, (10.0 * slots) ** (1.0 / 3.0))


def axis_steps(count):
    return ((0, False), (1, True)) if count == 2 else ((-1, False), (0, False), (1, False))


def shell(sizes):
    return list(itertools.product(*[axis_steps(count) for count in sizes]))


def own_cell():
    return [lax.axis_index(axis) for axis in AXES]


def linear(cell, steps, sizes):
    value = 0
    for coordinate, step, count in zip(cell, steps, sizes):
        value = value * count + (coordinate + (step % count)) % count
    return value


def around(cell, center, boxes, sizes):
    return [linear(cell, [center[a] + box[a][0] for a in range(3)], sizes) for box in boxes]


def fill_table(table, cell, boxes, sizes):
    for g, center in enumerate(CENTERS):
        for n, place in enumerate(around(cell, center, boxes, sizes)):
            table[g * len(boxes) + n] = place


def pieces_of(values):
    pieces = []
    for _ in range(3):
        piece = values.astype(BF16).astype(F32)
        pieces.append(piece)
        values = values - piece
    return pieces


def pick(blocks, hit):
    count = blocks.shape[0]
    stacked = jnp.concatenate(pieces_of(blocks), axis=0).astype(BF16)
    got = jnp.dot(stacked, hit, preferred_element_type=F32)
    return (got[0:count] + got[count : 2 * count]) + got[2 * count :]


def pack_kernel(sizes, slots, moves):
    devices = int(np.prod(sizes))

    def kernel(*refs):
        count, inputs, (send, own), staged, sems = refs[0], refs[1:9], refs[9:11], refs[11:19], refs[19]
        copies = [pltpu.make_async_copy(inputs[i], staged[i], sems.at[i]) for i in range(8)]
        for copy in copies:
            copy.start()
        for copy in copies:
            copy.wait()
        frac, vel, charge, drude, screen, label, mass, leaving = staged
        cell = own_cell()
        lane = lax.broadcasted_iota(jnp.int32, (1, slots), 1)
        live = lane < count[0]
        fr = jnp.concatenate([frac[a] for a in range(3)], axis=0)
        ve = jnp.concatenate([vel[a] for a in range(3)], axis=0)
        q = jnp.where(live, charge[...], 0.0)
        qd = jnp.where(live, drude[...], -1.0)
        sc = screen[...]
        lb = label[...].astype(F32)
        ms = mass[...]
        lv = jnp.concatenate([leaving[k].astype(F32) for k in range(6)], axis=0)
        lv = jnp.concatenate([lv, jnp.full((2, moves), -1.0, F32)], axis=0)
        spread = (
            lax.broadcasted_iota(jnp.int32, (moves, LANES), 1) % moves
            == lax.broadcasted_iota(jnp.int32, (moves, LANES), 0)
        ).astype(F32)
        repeated = jnp.dot(lv.astype(BF16), spread.astype(BF16), preferred_element_type=F32)
        slot_col = lax.broadcasted_iota(jnp.int32, (slots, LANES), 0).astype(F32)
        values = jnp.concatenate([ve, ms, jnp.zeros((4, slots), F32)], axis=0)
        field = lax.broadcasted_iota(jnp.int32, (8, LANES), 1) // moves - 1
        wanted = field == lax.broadcasted_iota(jnp.int32, (8, LANES), 0)
        first = lax.broadcasted_iota(jnp.int32, (1, LANES), 1) < moves
        statics = jnp.concatenate([fr, q, qd, sc, lb, jnp.zeros((1, slots), F32)], axis=0)
        send[...] = jnp.broadcast_to(statics[None], (devices, 8, slots))
        hits = jnp.concatenate(
            [(slot_col == repeated[k : k + 1]).astype(F32).astype(BF16) for k in range(6)], axis=1
        )
        picked = pick(values, hits)
        for k, unit in enumerate(UNITS):
            mine = picked[:, k * LANES : (k + 1) * LANES]
            row = jnp.sum(jnp.where(wanted, mine, 0.0), axis=0, keepdims=True)
            row = jnp.where(first, repeated[k : k + 1], row)
            side = (k % 2) * LANES
            send[linear(cell, unit, sizes), 7:8, side : side + LANES] = row
        ones = jnp.ones((16, 6 * LANES), BF16)
        departed = lax.dot_general(ones, hits, (((1,), (1,)), ((), ())), preferred_element_type=F32)[0:1]
        alive = live.astype(F32)
        gain = jnp.where(live, DRUDE_GAIN * qd, 0.0)
        own[...] = jnp.concatenate(
            [fr, q, qd, sc, lb, ms, ve, alive, jnp.where(departed > 0.5, 0.0, alive)]
            + [MOMENT * (gain * qd), gain, KICK * q / ms],
            axis=0,
        )

    return kernel


def columns(rows):
    lanes = rows.shape[1]
    padded = jnp.concatenate([rows, jnp.zeros((LANES - rows.shape[0], lanes), F32)], axis=0)
    return padded.T


def derived(fr, qd, sc, length):
    root = (DRUDE_GAIN**-0.5) / jnp.abs(qd)
    return fr * length, root, (0.25 * CUTOFF**3) * sc * root


def target_of(block, length, count):
    rows = block.shape[0]
    wide = [jnp.broadcast_to(block[:, c : c + 1], (rows, LANES)) for c in range(count)]
    shifted = [{-1: wide[a] + length, 0: wide[a], 1: wide[a] - length} for a in range(3)]
    return wide, shifted


def reader(source, place, half, rows):
    lanes = slice(half * LANES, (half + 1) * LANES)
    return lambda c: jnp.broadcast_to(source[place, c : c + 1, lanes], (rows, LANES))


def offsets(wide, shifted, row, box, length):
    deltas = []
    for a in range(3):
        step, nearest = box[a]
        if nearest:
            raw = wide[a] - row(a)
            deltas.append(raw - jnp.where(raw > 0.0, length, -length))
        else:
            deltas.append(shifted[a][step] - row(a))
    return deltas


def norm(deltas):
    return deltas[0] * deltas[0] + deltas[1] * deltas[1] + deltas[2] * deltas[2]


def terms(wide, dist_sq, row):
    inverse = lax.rsqrt(dist_sq)
    fade = inverse * jnp.maximum(1.0 - dist_sq, 0.0)
    half_x = (wide[3] * row(5) + wide[4] * row(4)) * (dist_sq * (dist_sq * inverse))
    tanh = jnp.tanh(half_x)
    root = fade * lax.rsqrt(1.0 + tanh)
    base = (root * root) * inverse
    return inverse, half_x, tanh, base


def charge_sum(fields, wide, deltas, direct, row):
    weight = jnp.where(wide[5] != row(6), direct, 0.0) * row(3)
    return [fields[a] + weight * deltas[a] for a in range(3)]


def image_list(boxes):
    first, rest = [], []
    for n, box in enumerate(boxes):
        combos = list(itertools.product(*[(1, -1) if nearest else (step,) for step, nearest in box]))
        first.append((n, combos[0]))
        rest.extend((n, combo) for combo in combos[1:])
    return first + rest


def is_center(box):
    return all(step == 0 for step, _ in box)


def rows_of(parts):
    return [jnp.sum(part.T, axis=0, keepdims=True) for part in parts]


def send_moments(send, moments, slots):
    halves = slots // LANES
    for a in range(3):
        for h in range(halves):
            row = moments[a][:, h * LANES : (h + 1) * LANES]
            send[:, a * halves + h] = jnp.broadcast_to(row[None], (send.shape[0], 1, LANES))


def split(values, high, low, spot):
    high[spot, :] = values.astype(BF16)
    low[spot, :] = (values - high[spot, :].astype(F32)).astype(BF16)


def field_kernel(sizes, slots, tile):
    boxes = shell(sizes)
    images = image_list(boxes)
    length = box_length(slots) / CUTOFF

    def kernel(recv, own, source, frames, ahi, alo, bhi, blo, perm, send, chosen, cols, acc, ready):
        fr, root, part = derived(recv[:, 0:3, :], recv[:, 4:5, :], recv[:, 5:6, :], length)
        source[:, 0:3, :] = fr
        source[:, 3:4, :] = (2.0 / CUTOFF**2) * recv[:, 3:4, :]
        source[:, 4:5, :] = root
        source[:, 5:6, :] = part
        source[:, 6:8, :] = recv[:, 6:8, :]
        places = around(own_cell(), CENTERS[0], boxes, sizes)
        for n in range(len(boxes)):
            chosen[n] = source[places[n]]
        for n in range(len(boxes), chosen.shape[0]):
            chosen[n] = jnp.zeros((8, slots), F32)
        group = LANES // 8
        for g in range(chosen.shape[0] // group):
            cols[:, g * LANES : (g + 1) * LANES] = chosen[g * group : (g + 1) * group].reshape(LANES, slots).T
        one = jnp.ones((1, slots), F32)
        for m, (n, step) in enumerate(images):
            spots = [chosen[n, a : a + 1, :] + (step[a] - 0.5) * length for a in range(3)]
            frames[m] = jnp.concatenate(spots + [one] + spots + [one], axis=0)
        fr, root, part = derived(own[0:3], own[4:5], own[5:6], length)
        wide = [jnp.broadcast_to(row, (tile, slots)) for row in (fr[0:1], fr[1:2], fr[2:3], root, part, own[6:7])]
        acc[...] = jnp.zeros(acc.shape, F32)

        def body(t, carry):
            at = pl.ds(pl.multiple_of(t * tile, tile), tile)
            block = cols[at, :]
            after = pl.ds(pl.multiple_of(jnp.minimum(t + 1, slots // tile - 1) * tile, tile), tile)
            upcoming = cols[after, :]
            fields = [acc[a] for a in range(3)]
            for n, box in enumerate(boxes):
                if n == 0:
                    row = lambda c: jnp.concatenate([ready[c]] * (slots // LANES), axis=1)
                else:
                    row = lambda c: jnp.broadcast_to(block[:, n * 8 + c : n * 8 + c + 1], (tile, slots))
                deltas, ahead = [], []
                for a in range(3):
                    step, nearest = box[a]
                    raw = wide[a] - row(a) if nearest or not step else (wide[a] - step * length) - row(a)
                    if nearest:
                        ahead.append((a, raw > 0.0))
                        raw = raw - jnp.where(ahead[-1][1], length, -length)
                    deltas.append(raw)
                dist_sq = norm(deltas)
                if is_center(box):
                    target = lax.broadcasted_iota(jnp.int32, (tile, slots), 1)
                    keep = target != lax.broadcasted_iota(jnp.int32, (tile, slots), 0) + t * tile
                    dist_sq = jnp.where(keep, dist_sq, 1.0)
                inverse, half_x, tanh, base = terms(wide, dist_sq, row)
                direct = base * tanh
                weight = jnp.where(wide[5] != row(6), direct, 0.0) * row(3)
                fields = [
                    fields[a] + jnp.sum((weight * deltas[a]).reshape(tile // 8, 8, slots), axis=0)
                    for a in range(3)
                ]
                radial = base * (inverse * inverse) * (tanh - half_x * (1.0 - tanh))
                if is_center(box):
                    direct = jnp.where(keep, direct, 0.0)
                    radial = jnp.where(keep, radial, 0.0)
                spot = pl.ds(pl.multiple_of(n * slots + t * tile, tile), tile)
                split(direct, bhi, blo, spot)
                for m, (owner, step) in enumerate(images):
                    if owner != n:
                        continue
                    part = radial
                    for a, side in ahead:
                        part = jnp.where(side, part, 0.0) if step[a] > 0 else jnp.where(side, 0.0, part)
                    spot = pl.ds(pl.multiple_of(m * slots + t * tile, tile), tile)
                    split(part, ahi, alo, spot)
            for a in range(3):
                acc[a] = fields[a]
            for c in range(7):
                ready[c] = jnp.broadcast_to(upcoming[:, c : c + 1], (tile, LANES))
            return carry

        for c in range(7):
            ready[c] = jnp.broadcast_to(cols[0:tile, c : c + 1], (tile, LANES))

        lax.fori_loop(0, slots // tile, body, 0)
        rows = [jnp.sum(acc[a], axis=0, keepdims=True) for a in range(3)]
        perm[...] = jnp.concatenate(rows, axis=0)
        send_moments(send, [own[13:14] * row for row in rows], slots)

    return kernel


def build_lhs(lhs, recv, frames, places, images, slots):
    halves = slots // LANES
    upper = lax.broadcasted_iota(jnp.int32, (8, slots), 0) < 4
    known = {}
    for m, (n, _) in enumerate(images):
        if n not in known:
            known[n] = [
                jnp.concatenate(
                    [recv[places[n], a * halves + h] for h in range(halves)], axis=1
                )
                for a in range(3)
            ]
        mu = known[n]
        along = frames[m, 0:1, :] * mu[0] + frames[m, 1:2, :] * mu[1] + frames[m, 2:3, :] * mu[2]
        frame = frames[m]
        whole = lambda row: jnp.broadcast_to(row, (8, slots))
        value = jnp.concatenate(
            [
                frame * jnp.where(upper, whole(mu[0]), whole(mu[1])),
                frame * jnp.where(upper, whole(mu[2]), whole(along)),
            ],
            axis=0,
        )
        lanes = slice(m * slots, (m + 1) * slots)
        for piece in range(3):
            high = value.astype(BF16)
            lhs[piece * 16 : (piece + 1) * 16, lanes] = high
            value = value - high.astype(F32)


def product(lhs, high, low, at):
    left = lhs[:, at]
    dot = lambda right: jnp.dot(left, right[at, :], preferred_element_type=F32)
    return dot(high) + dot(low)


def induced_rows(tensor, plain, own, perm, slots):
    length = box_length(slots) / CUTOFF
    tensor = 3.0 * (tensor[0:16] + (tensor[16:32] + tensor[32:48]))
    plain = plain[0:16] + (plain[16:32] + plain[32:48])
    spot = [(own[a : a + 1] - 0.5) * length for a in range(3)]
    first = [tensor[4 * a + 3 : 4 * a + 4] for a in range(3)]
    along = spot[0] * first[0] + spot[1] * first[1] + spot[2] * first[2] - tensor[15:16]
    rows = []
    for a in range(3):
        mixed = sum(tensor[4 * b + a : 4 * b + a + 1] * spot[b] for b in range(3))
        value = (spot[a] * along - mixed) + tensor[12 + a : 13 + a]
        rows.append(perm[a : a + 1] + (value - plain[4 * a + 3 : 4 * a + 4]))
    return rows


def arrival_records(first_recv, origin, moves, slots):
    lane = lax.broadcasted_iota(jnp.int32, (1, LANES), 1)
    extra = jnp.full((8, LANES), -1.0, F32)
    for k in range(6):
        side = (k % 2) * LANES
        row = first_recv[origin[k], 7:8, side : side + LANES]
        row = jnp.broadcast_to(row, (8, LANES))
        fields = [pltpu.roll(row, (k * moves - c * moves) % LANES, 1)[0:1] for c in range(5)]
        block = jnp.concatenate(fields + [extra[0:3]], axis=0)
        extra = jnp.where(lane // moves == k, block, extra)
    slot = extra[0:1]
    slot_col = lax.broadcasted_iota(jnp.int32, (slots, LANES), 0).astype(F32)
    hit = (slot_col == slot).astype(F32).astype(BF16)
    taken = pick(jnp.concatenate([first_recv[origin[k]] for k in range(6)], axis=0), hit)
    got = jnp.zeros((8, LANES), F32)
    for k in range(6):
        got = jnp.where(lane // moves == k, taken[8 * k : 8 * k + 8], got)
    return got, extra, hit


def induced_kernel(sizes, slots, moves, prepare):
    boxes = shell(sizes)
    images = image_list(boxes)
    length = box_length(slots) / CUTOFF

    def kernel(recv, frames, ahi, alo, bhi, blo, own, perm, *rest):
        if prepare:
            first_recv, send, shift, arrive, hits, targets, lhs = rest
        else:
            send, shift, lhs = rest
        cell = own_cell()
        places = around(cell, CENTERS[0], boxes, sizes)
        build_lhs(lhs, recv, frames, places, images, slots)
        tensor = product(lhs, ahi, alo, slice(0, len(images) * slots))
        plain = product(lhs, bhi, blo, slice(0, len(boxes) * slots))
        rows = induced_rows(tensor, plain, own, perm, slots)
        shift[...] = jnp.concatenate([own[14:15] * row for row in rows], axis=0)
        send_moments(send, [own[13:14] * row for row in rows], slots)
        if prepare:
            origin = [linear(cell, [-step for step in unit], sizes) for unit in UNITS]
            got, extra, hit = arrival_records(first_recv, origin, moves, slots)
            arrive[0:8] = got
            arrive[8:16] = extra
            hits[...] = hit
            slot = extra[0:1]
            fr, root, part = derived(got[0:3], jnp.where(slot >= 0.0, got[4:5], -1.0), got[5:6], length)
            cols = columns(jnp.concatenate([fr, root, part, got[6:7], slot, slot], axis=0))
            for k in range(6):
                for c, value in enumerate(target_of(cols[k * moves : (k + 1) * moves], length, 7)[0]):
                    targets[k, c] = value

    return kernel


def final_kernel(sizes, slots, moves):
    boxes = shell(sizes)
    images = image_list(boxes)
    tile = moves
    halves = slots // LANES
    edge = box_length(slots)
    length = edge / CUTOFF

    def kernel(
        recv, frames, ahi, alo, bhi, blo, own, perm, shift, source, arrive, hits, targets,
        staying, arrivals, lhs, sums, acc, table, out_stay, out_come, out_sems,
    ):
        cell = own_cell()
        places = around(cell, CENTERS[0], boxes, sizes)
        build_lhs(lhs, recv, frames, places, images, slots)
        fill_table(table, cell, boxes, sizes)
        lane = lax.broadcasted_iota(jnp.int32, (1, LANES), 1)
        origin = [linear(cell, [-step for step in unit], sizes) for unit in UNITS]
        blank = jnp.zeros((5, slots), F32)
        blocks = []
        for k in range(6):
            for a in range(3):
                blocks.append(
                    jnp.concatenate([recv[origin[k], a * halves + h] for h in range(halves)], axis=1)
                )
            blocks.append(blank)
        taken = pick(jnp.concatenate(blocks, axis=0), hits[...])
        moment = jnp.zeros((8, LANES), F32)
        for k in range(6):
            moment = jnp.where(lane // moves == k, taken[8 * k : 8 * k + 8], moment)
        got = arrive[0:8]
        extra = arrive[8:16]
        present = extra[0:1] >= 0.0
        acc[...] = jnp.zeros(acc.shape, F32)
        steps = [len(images) // 6 * slots, len(boxes) // 6 * slots]
        for which, (high, low, count) in enumerate(((ahi, alo, len(images)), (bhi, blo, len(boxes)))):
            sums[which] = jnp.zeros((48, slots), F32)
            if count * slots > 6 * steps[which]:
                sums[which] = product(lhs, high, low, slice(6 * steps[which], count * slots))

        def incoming(k, carry):
            for which, (high, low) in enumerate(((ahi, alo), (bhi, blo))):
                part = pl.ds(pl.multiple_of(k * steps[which], LANES), steps[which])
                sums[which] = sums[which] + product(lhs, high, low, part)
            at = pl.ds(pl.multiple_of(k * tile, tile), tile)
            wide = [targets[k, c] for c in range(7)]
            shifted = [{-1: wide[a] + length, 0: wide[a], 1: wide[a] - length} for a in range(3)]
            fields = [jnp.zeros((tile, LANES), F32)] * 3
            for n, box in enumerate(boxes):
                spot = table[(k + 1) * len(boxes) + n]
                for half in range(halves):
                    row = reader(source, spot, half, tile)
                    mu = [
                        jnp.broadcast_to(recv[spot, a * halves + half], (tile, LANES))
                        for a in range(3)
                    ]
                    deltas = offsets(wide, shifted, row, box, length)
                    dist_sq = norm(deltas)
                    if is_center(box):
                        ids = lax.broadcasted_iota(jnp.int32, (tile, LANES), 1) + half * LANES
                        keep = wide[6] != ids.astype(F32)
                        dist_sq = jnp.where(keep, dist_sq, 1.0)
                    inverse, half_x, tanh, base = terms(wide, dist_sq, row)
                    direct = base * tanh
                    radial = base * (inverse * inverse) * (tanh - half_x * (1.0 - tanh))
                    if is_center(box):
                        direct = jnp.where(keep, direct, 0.0)
                        radial = jnp.where(keep, radial, 0.0)
                    pull = jnp.where(wide[5] != row(6), direct, 0.0) * row(3)
                    pull = pull + (3.0 * radial) * (deltas[0] * mu[0] + deltas[1] * mu[1] + deltas[2] * mu[2])
                    fields = [fields[a] + (pull * deltas[a] - direct * mu[a]) for a in range(3)]
            for a in range(3):
                acc[a, at, :] = fields[a]
            return carry

        lax.fori_loop(0, 6, incoming, 0)
        field = induced_rows(sums[0], sums[1], own, perm, slots)
        remain = own[12:13] > 0.5
        fast = [own[8 + a : 9 + a] + own[15:16] * field[a] for a in range(3)]
        place = [own[a : a + 1] + TIMESTEP * fast[a] / edge for a in range(3)]
        drude = [shift[a : a + 1] for a in range(3)]
        for r, row in enumerate(place + fast + drude):
            out_stay[r] = jnp.where(remain, row, 0.0)
        early = pltpu.make_async_copy(out_stay, staying, out_sems.at[0])
        early.start()

        pull = rows_of([acc[a] for a in range(3)])
        q = got[3:4]
        qd = got[4:5]
        mass = jnp.where(present, extra[4:5], 1.0)
        gain = KICK * q / mass
        fast = [extra[1 + a : 2 + a] + gain * pull[a] for a in range(3)]
        place = [got[a : a + 1] + TIMESTEP * fast[a] / edge for a in range(3)]
        for k, unit in enumerate(UNITS):
            for a in range(3):
                if unit[a]:
                    place[a] = place[a] - jnp.where(lane // moves == k, float(unit[a]), 0.0)
        safe = jnp.where(present, qd, -1.0) * MOMENT
        drude = [moment[a : a + 1] / safe for a in range(3)]
        record = place + fast + drude + [q, qd, got[5:6], got[6:7], mass]
        for r, row in enumerate(record):
            out_come[r] = jnp.where(present, row, 0.0)[:, 0 : 6 * moves]
        late = pltpu.make_async_copy(out_come, arrivals, out_sems.at[1])
        late.start()
        early.wait()
        late.wait()

    return kernel


def solution(mesh):
    sizes = tuple(mesh.shape[axis] for axis in AXES)
    devices = int(np.prod(sizes))
    boxes = shell(sizes)
    count_boxes = len(boxes)
    count_images = len(image_list(boxes))
    padded_boxes = -(-count_boxes // 16) * 16

    def local(fractions, velocity, charge, drude_charge, screening, labels, masses, counts, leaving):
        slots = charge.shape[-1]
        moves = leaving.shape[-1]
        exchange = lambda block: lax.all_to_all(block, AXES, 0, 0)
        shape = lambda *dims: jax.ShapeDtypeStruct(dims, F32)
        half = lambda *dims: jax.ShapeDtypeStruct(dims, BF16)
        hbm = lambda x: pltpu.with_memory_space_constraint(x, pltpu.HBM)
        moment_shape = (devices, 3 * (slots // LANES), 1, LANES)
        dma = pltpu.SemaphoreType.DMA

        def call(kernel, in_specs, outs, out_specs, scratch, flops, limit):
            return pl.pallas_call(
                kernel,
                in_specs=in_specs,
                out_shape=outs,
                out_specs=out_specs,
                scratch_shapes=scratch,
                compiler_params=pltpu.CompilerParams(vmem_limit_bytes=limit),
                cost_estimate=pl.CostEstimate(flops=flops, bytes_accessed=1 << 20, transcendentals=0),
            )

        flat = [
            fractions.reshape(3, 1, slots),
            velocity.reshape(3, 1, slots),
            charge.reshape(1, slots),
            drude_charge.reshape(1, slots),
            screening.reshape(1, slots),
            labels.reshape(1, slots),
            masses.reshape(1, slots),
            leaving.reshape(6, 1, moves),
        ]
        send, own = call(
            pack_kernel(sizes, slots, moves),
            [smem()] + [anywhere()] * 8,
            (shape(devices, 8, slots), shape(16, slots)),
            (vmem(), vmem()),
            [VMEM(array.shape, array.dtype) for array in flat] + [dma((8,))],
            1 << 20,
            8 << 20,
        )(counts.reshape(1), *[hbm(x) for x in flat])
        first = exchange(send)
        outs = (
            shape(devices, 8, slots),
            shape(count_images, 8, slots),
            half(count_images * slots, slots),
            half(count_images * slots, slots),
            half(count_boxes * slots, slots),
            half(count_boxes * slots, slots),
            shape(3, slots),
            shape(*moment_shape),
        )
        source, frames, ahi, alo, bhi, blo, perm, moments = call(
            field_kernel(sizes, slots, 32),
            [vmem()] * 2,
            outs,
            (vmem(),) * len(outs),
            [
                VMEM((padded_boxes, 8, slots), F32),
                VMEM((slots, padded_boxes * 8), F32),
                VMEM((3, 8, slots), F32),
                VMEM((7, 32, LANES), F32),
            ],
            1 << 25,
            8 << 20,
        )(first, own)
        got = exchange(moments)
        tensors = (frames, ahi, alo, bhi, blo, own, perm)
        lhs = VMEM((48, count_images * slots), BF16)
        for step in range(ITERS - 1):
            prepare = step == ITERS - 2
            outs = (shape(*moment_shape), shape(3, slots))
            if prepare:
                outs = outs + (shape(16, LANES), half(slots, LANES), shape(6, 7, moves, LANES))
            moments, shift, *arriving = call(
                induced_kernel(sizes, slots, moves, prepare),
                [vmem()] * (9 if prepare else 8),
                outs,
                (vmem(),) * len(outs),
                [lhs],
                1 << 24,
                4 << 20,
            )(got, *tensors, *((first,) if prepare else ()))
            got = exchange(moments)
        staying, arrivals = call(
            final_kernel(sizes, slots, moves),
            [vmem()] * 13,
            (pltpu.HBM((9, 1, slots), F32), pltpu.HBM((14, 1, 6 * moves), F32)),
            (anywhere(), anywhere()),
            [
                lhs,
                VMEM((2, 48, slots), F32),
                VMEM((3, LANES, LANES), F32),
                pltpu.SMEM((len(CENTERS) * count_boxes,), jnp.int32),
                VMEM((9, 1, slots), F32),
                VMEM((14, 1, 6 * moves), F32),
                dma((2,)),
            ],
            1 << 24,
            8 << 20,
        )(got, *tensors, shift, source, *arriving)
        return staying.reshape(1, 1, 1, 9, slots), arrivals.reshape(1, 1, 1, 14, 6 * moves)

    box = P("gx", "gy", "gz", None)
    rows = P("gx", "gy", "gz", None, None)
    return jax.shard_map(
        local,
        mesh=mesh,
        in_specs=(rows, rows, box, box, box, box, box, P("gx", "gy", "gz"), rows),
        out_specs=(rows, rows),
        check_vma=False,
    )
```

```python
import itertools

import jax
import jax.numpy as jnp
import numpy as np
from jax import lax
from jax.experimental import pallas as pl
from jax.experimental.pallas import tpu as pltpu
from jax.sharding import PartitionSpec as P

ITERS = 3
CUTOFF = 12.0
DRUDE_GAIN = 0.3320636
KICK = 0.002 * 418.4 * 332.0636
TIMESTEP = 0.002
UNITS = ((1, 0, 0), (-1, 0, 0), (0, 1, 0), (0, -1, 0), (0, 0, 1), (0, 0, -1))
AXES = ("gx", "gy", "gz")
LANES = 128
CENTERS = ((0, 0, 0),) + tuple(tuple(-step for step in unit) for unit in UNITS)
MOMENT = 2.0 / CUTOFF**3
F32 = jnp.float32
BF16 = jnp.bfloat16
VMEM = pltpu.VMEM


def vmem():
    return pl.BlockSpec(memory_space=pltpu.VMEM)


def smem():
    return pl.BlockSpec(memory_space=pltpu.SMEM)


def anywhere():
    return pl.BlockSpec(memory_space=pltpu.HBM)


def box_length(slots):
    return max(12.0, (10.0 * slots) ** (1.0 / 3.0))


def axis_steps(count):
    return ((0, False), (1, True)) if count == 2 else ((-1, False), (0, False), (1, False))


def shell(sizes):
    return list(itertools.product(*[axis_steps(count) for count in sizes]))


def own_cell():
    return [lax.axis_index(axis) for axis in AXES]


def linear(cell, steps, sizes):
    value = 0
    for coordinate, step, count in zip(cell, steps, sizes):
        value = value * count + (coordinate + (step % count)) % count
    return value


def around(cell, center, boxes, sizes):
    return [linear(cell, [center[a] + box[a][0] for a in range(3)], sizes) for box in boxes]


def fill_table(table, cell, boxes, sizes):
    for g, center in enumerate(CENTERS):
        for n, place in enumerate(around(cell, center, boxes, sizes)):
            table[g * len(boxes) + n] = place


def pieces_of(values):
    pieces = []
    for _ in range(3):
        piece = values.astype(BF16).astype(F32)
        pieces.append(piece)
        values = values - piece
    return pieces


def pick(blocks, hit):
    count = blocks.shape[0]
    stacked = jnp.concatenate(pieces_of(blocks), axis=0).astype(BF16)
    got = jnp.dot(stacked, hit, preferred_element_type=F32)
    return (got[0:count] + got[count : 2 * count]) + got[2 * count :]


def pack_kernel(sizes, slots, moves):
    devices = int(np.prod(sizes))

    def kernel(*refs):
        count, inputs, (send, own), staged, sems = refs[0], refs[1:9], refs[9:11], refs[11:19], refs[19]
        copies = [pltpu.make_async_copy(inputs[i], staged[i], sems.at[i]) for i in range(8)]
        for copy in copies:
            copy.start()
        for copy in copies:
            copy.wait()
        frac, vel, charge, drude, screen, label, mass, leaving = staged
        cell = own_cell()
        lane = lax.broadcasted_iota(jnp.int32, (1, slots), 1)
        live = lane < count[0]
        fr = jnp.concatenate([frac[a] for a in range(3)], axis=0)
        ve = jnp.concatenate([vel[a] for a in range(3)], axis=0)
        q = jnp.where(live, charge[...], 0.0)
        qd = jnp.where(live, drude[...], -1.0)
        sc = screen[...]
        lb = label[...].astype(F32)
        ms = mass[...]
        lv = jnp.concatenate([leaving[k].astype(F32) for k in range(6)], axis=0)
        lv = jnp.concatenate([lv, jnp.full((2, moves), -1.0, F32)], axis=0)
        spread = (
            lax.broadcasted_iota(jnp.int32, (moves, LANES), 1) % moves
            == lax.broadcasted_iota(jnp.int32, (moves, LANES), 0)
        ).astype(F32)
        repeated = jnp.dot(lv.astype(BF16), spread.astype(BF16), preferred_element_type=F32)
        slot_col = lax.broadcasted_iota(jnp.int32, (slots, LANES), 0).astype(F32)
        values = jnp.concatenate([ve, ms, jnp.zeros((4, slots), F32)], axis=0)
        field = lax.broadcasted_iota(jnp.int32, (8, LANES), 1) // moves - 1
        wanted = field == lax.broadcasted_iota(jnp.int32, (8, LANES), 0)
        first = lax.broadcasted_iota(jnp.int32, (1, LANES), 1) < moves
        statics = jnp.concatenate([fr, q, qd, sc, lb, jnp.zeros((1, slots), F32)], axis=0)
        send[...] = jnp.broadcast_to(statics[None], (devices, 8, slots))
        hits = jnp.concatenate(
            [(slot_col == repeated[k : k + 1]).astype(F32).astype(BF16) for k in range(6)], axis=1
        )
        picked = pick(values, hits)
        for k, unit in enumerate(UNITS):
            mine = picked[:, k * LANES : (k + 1) * LANES]
            row = jnp.sum(jnp.where(wanted, mine, 0.0), axis=0, keepdims=True)
            row = jnp.where(first, repeated[k : k + 1], row)
            side = (k % 2) * LANES
            send[linear(cell, unit, sizes), 7:8, side : side + LANES] = row
        ones = jnp.ones((16, 6 * LANES), BF16)
        departed = lax.dot_general(ones, hits, (((1,), (1,)), ((), ())), preferred_element_type=F32)[0:1]
        alive = live.astype(F32)
        gain = jnp.where(live, DRUDE_GAIN * qd, 0.0)
        own[...] = jnp.concatenate(
            [fr, q, qd, sc, lb, ms, ve, alive, jnp.where(departed > 0.5, 0.0, alive)]
            + [MOMENT * (gain * qd), gain, KICK * q / ms],
            axis=0,
        )

    return kernel


def columns(rows):
    lanes = rows.shape[1]
    padded = jnp.concatenate([rows, jnp.zeros((LANES - rows.shape[0], lanes), F32)], axis=0)
    return padded.T


def derived(fr, qd, sc, length):
    root = (DRUDE_GAIN**-0.5) / jnp.abs(qd)
    return fr * length, root, (0.25 * CUTOFF**3) * sc * root


def target_of(block, length, count):
    rows = block.shape[0]
    wide = [jnp.broadcast_to(block[:, c : c + 1], (rows, LANES)) for c in range(count)]
    shifted = [{-1: wide[a] + length, 0: wide[a], 1: wide[a] - length} for a in range(3)]
    return wide, shifted


def reader(source, place, half, rows):
    lanes = slice(half * LANES, (half + 1) * LANES)
    return lambda c: jnp.broadcast_to(source[place, c : c + 1, lanes], (rows, LANES))


def offsets(wide, shifted, row, box, length):
    deltas = []
    for a in range(3):
        step, nearest = box[a]
        if nearest:
            raw = wide[a] - row(a)
            deltas.append(raw - jnp.where(raw > 0.0, length, -length))
        else:
            deltas.append(shifted[a][step] - row(a))
    return deltas


def norm(deltas):
    return deltas[0] * deltas[0] + deltas[1] * deltas[1] + deltas[2] * deltas[2]


def terms(wide, dist_sq, row):
    inverse = lax.rsqrt(dist_sq)
    fade = inverse * jnp.maximum(1.0 - dist_sq, 0.0)
    half_x = (wide[3] * row(5) + wide[4] * row(4)) * (dist_sq * (dist_sq * inverse))
    tanh = jnp.tanh(half_x)
    root = fade * lax.rsqrt(1.0 + tanh)
    base = (root * root) * inverse
    return inverse, half_x, tanh, base


def charge_sum(fields, wide, deltas, direct, row):
    weight = jnp.where(wide[5] != row(6), direct, 0.0) * row(3)
    return [fields[a] + weight * deltas[a] for a in range(3)]


def image_list(boxes):
    first, rest = [], []
    for n, box in enumerate(boxes):
        combos = list(itertools.product(*[(1, -1) if nearest else (step,) for step, nearest in box]))
        first.append((n, combos[0]))
        rest.extend((n, combo) for combo in combos[1:])
    return first + rest


def is_center(box):
    return all(step == 0 for step, _ in box)


def rows_of(parts):
    return [jnp.sum(part.T, axis=0, keepdims=True) for part in parts]


def send_moments(send, moments, slots):
    halves = slots // LANES
    for a in range(3):
        for h in range(halves):
            row = moments[a][:, h * LANES : (h + 1) * LANES]
            send[:, a * halves + h] = jnp.broadcast_to(row[None], (send.shape[0], 1, LANES))


def split(values, high, low, spot):
    high[spot, :] = values.astype(BF16)
    low[spot, :] = (values - high[spot, :].astype(F32)).astype(BF16)


def field_kernel(sizes, slots, tile):
    boxes = shell(sizes)
    images = image_list(boxes)
    length = box_length(slots) / CUTOFF

    def kernel(recv, own, source, frames, ahi, alo, bhi, blo, perm, send, chosen, cols, acc, ready):
        fr, root, part = derived(recv[:, 0:3, :], recv[:, 4:5, :], recv[:, 5:6, :], length)
        source[:, 0:3, :] = fr
        source[:, 3:4, :] = (2.0 / CUTOFF**2) * recv[:, 3:4, :]
        source[:, 4:5, :] = root
        source[:, 5:6, :] = part
        source[:, 6:8, :] = recv[:, 6:8, :]
        places = around(own_cell(), CENTERS[0], boxes, sizes)
        for n in range(len(boxes)):
            chosen[n] = source[places[n]]
        for n in range(len(boxes), chosen.shape[0]):
            chosen[n] = jnp.zeros((8, slots), F32)
        group = LANES // 8
        for g in range(chosen.shape[0] // group):
            cols[:, g * LANES : (g + 1) * LANES] = chosen[g * group : (g + 1) * group].reshape(LANES, slots).T
        one = jnp.ones((1, slots), F32)
        for m, (n, step) in enumerate(images):
            spots = [chosen[n, a : a + 1, :] + (step[a] - 0.5) * length for a in range(3)]
            frames[m] = jnp.concatenate(spots + [one] + spots + [one], axis=0)
        fr, root, part = derived(own[0:3], own[4:5], own[5:6], length)
        wide = [jnp.broadcast_to(row, (tile, slots)) for row in (fr[0:1], fr[1:2], fr[2:3], root, part, own[6:7])]
        acc[...] = jnp.zeros(acc.shape, F32)

        def body(t, carry):
            at = pl.ds(pl.multiple_of(t * tile, tile), tile)
            block = cols[at, :]
            after = pl.ds(pl.multiple_of(jnp.minimum(t + 1, slots // tile - 1) * tile, tile), tile)
            upcoming = cols[after, :]
            fields = [acc[a] for a in range(3)]
            for n, box in enumerate(boxes):
                if n == 0:
                    row = lambda c: jnp.concatenate([ready[c]] * (slots // LANES), axis=1)
                else:
                    row = lambda c: jnp.broadcast_to(block[:, n * 8 + c : n * 8 + c + 1], (tile, slots))
                deltas, ahead = [], []
                for a in range(3):
                    step, nearest = box[a]
                    raw = wide[a] - row(a) if nearest or not step else (wide[a] - step * length) - row(a)
                    if nearest:
                        ahead.append((a, raw > 0.0))
                        raw = raw - jnp.where(ahead[-1][1], length, -length)
                    deltas.append(raw)
                dist_sq = norm(deltas)
                if is_center(box):
                    target = lax.broadcasted_iota(jnp.int32, (tile, slots), 1)
                    keep = target != lax.broadcasted_iota(jnp.int32, (tile, slots), 0) + t * tile
                    dist_sq = jnp.where(keep, dist_sq, 1.0)
                inverse, half_x, tanh, base = terms(wide, dist_sq, row)
                direct = base * tanh
                weight = jnp.where(wide[5] != row(6), direct, 0.0) * row(3)
                fields = [
                    fields[a] + jnp.sum((weight * deltas[a]).reshape(tile // 8, 8, slots), axis=0)
                    for a in range(3)
                ]
                radial = (inverse * inverse) * (direct - half_x * (base - direct))
                if is_center(box):
                    direct = jnp.where(keep, direct, 0.0)
                    radial = jnp.where(keep, radial, 0.0)
                spot = pl.ds(pl.multiple_of(n * slots + t * tile, tile), tile)
                split(direct, bhi, blo, spot)
                for m, (owner, step) in enumerate(images):
                    if owner != n:
                        continue
                    part = radial
                    for a, side in ahead:
                        part = jnp.where(side, part, 0.0) if step[a] > 0 else jnp.where(side, 0.0, part)
                    spot = pl.ds(pl.multiple_of(m * slots + t * tile, tile), tile)
                    split(part, ahi, alo, spot)
            for a in range(3):
                acc[a] = fields[a]
            for c in range(7):
                ready[c] = jnp.broadcast_to(upcoming[:, c : c + 1], (tile, LANES))
            return carry

        for c in range(7):
            ready[c] = jnp.broadcast_to(cols[0:tile, c : c + 1], (tile, LANES))

        lax.fori_loop(0, slots // tile, body, 0)
        rows = [jnp.sum(acc[a], axis=0, keepdims=True) for a in range(3)]
        perm[...] = jnp.concatenate(rows, axis=0)
        send_moments(send, [own[13:14] * row for row in rows], slots)

    return kernel


def build_lhs(lhs, recv, frames, places, images, slots):
    halves = slots // LANES
    upper = lax.broadcasted_iota(jnp.int32, (8, slots), 0) < 4
    known = {}
    for m, (n, _) in enumerate(images):
        if n not in known:
            known[n] = [
                jnp.concatenate(
                    [recv[places[n], a * halves + h] for h in range(halves)], axis=1
                )
                for a in range(3)
            ]
        mu = known[n]
        along = frames[m, 0:1, :] * mu[0] + frames[m, 1:2, :] * mu[1] + frames[m, 2:3, :] * mu[2]
        frame = frames[m]
        whole = lambda row: jnp.broadcast_to(row, (8, slots))
        value = jnp.concatenate(
            [
                frame * jnp.where(upper, whole(mu[0]), whole(mu[1])),
                frame * jnp.where(upper, whole(mu[2]), whole(along)),
            ],
            axis=0,
        )
        lanes = slice(m * slots, (m + 1) * slots)
        for piece in range(3):
            high = value.astype(BF16)
            lhs[piece * 16 : (piece + 1) * 16, lanes] = high
            value = value - high.astype(F32)


def product(lhs, high, low, at):
    left = lhs[:, at]
    dot = lambda right: jnp.dot(left, right[at, :], preferred_element_type=F32)
    return dot(high) + dot(low)


def induced_rows(tensor, plain, own, perm, slots):
    length = box_length(slots) / CUTOFF
    tensor = 3.0 * (tensor[0:16] + (tensor[16:32] + tensor[32:48]))
    plain = plain[0:16] + (plain[16:32] + plain[32:48])
    spot = [(own[a : a + 1] - 0.5) * length for a in range(3)]
    first = [tensor[4 * a + 3 : 4 * a + 4] for a in range(3)]
    along = spot[0] * first[0] + spot[1] * first[1] + spot[2] * first[2] - tensor[15:16]
    rows = []
    for a in range(3):
        mixed = sum(tensor[4 * b + a : 4 * b + a + 1] * spot[b] for b in range(3))
        value = (spot[a] * along - mixed) + tensor[12 + a : 13 + a]
        rows.append(perm[a : a + 1] + (value - plain[4 * a + 3 : 4 * a + 4]))
    return rows


def arrival_records(first_recv, origin, moves, slots):
    lane = lax.broadcasted_iota(jnp.int32, (1, LANES), 1)
    extra = jnp.full((8, LANES), -1.0, F32)
    for k in range(6):
        side = (k % 2) * LANES
        row = first_recv[origin[k], 7:8, side : side + LANES]
        row = jnp.broadcast_to(row, (8, LANES))
        fields = [pltpu.roll(row, (k * moves - c * moves) % LANES, 1)[0:1] for c in range(5)]
        block = jnp.concatenate(fields + [extra[0:3]], axis=0)
        extra = jnp.where(lane // moves == k, block, extra)
    slot = extra[0:1]
    slot_col = lax.broadcasted_iota(jnp.int32, (slots, LANES), 0).astype(F32)
    hit = (slot_col == slot).astype(F32).astype(BF16)
    taken = pick(jnp.concatenate([first_recv[origin[k]] for k in range(6)], axis=0), hit)
    got = jnp.zeros((8, LANES), F32)
    for k in range(6):
        got = jnp.where(lane // moves == k, taken[8 * k : 8 * k + 8], got)
    return got, extra, hit


def induced_kernel(sizes, slots, moves, prepare):
    boxes = shell(sizes)
    images = image_list(boxes)
    length = box_length(slots) / CUTOFF

    def kernel(recv, frames, ahi, alo, bhi, blo, own, perm, *rest):
        if prepare:
            first_recv, send, shift, arrive, hits, targets, lhs = rest
        else:
            send, shift, lhs = rest
        cell = own_cell()
        places = around(cell, CENTERS[0], boxes, sizes)
        build_lhs(lhs, recv, frames, places, images, slots)
        tensor = product(lhs, ahi, alo, slice(0, len(images) * slots))
        plain = product(lhs, bhi, blo, slice(0, len(boxes) * slots))
        rows = induced_rows(tensor, plain, own, perm, slots)
        shift[...] = jnp.concatenate([own[14:15] * row for row in rows], axis=0)
        send_moments(send, [own[13:14] * row for row in rows], slots)
        if prepare:
            origin = [linear(cell, [-step for step in unit], sizes) for unit in UNITS]
            got, extra, hit = arrival_records(first_recv, origin, moves, slots)
            arrive[0:8] = got
            arrive[8:16] = extra
            hits[...] = hit
            slot = extra[0:1]
            fr, root, part = derived(got[0:3], jnp.where(slot >= 0.0, got[4:5], -1.0), got[5:6], length)
            cols = columns(jnp.concatenate([fr, root, part, got[6:7], slot, slot], axis=0))
            for k in range(6):
                for c, value in enumerate(target_of(cols[k * moves : (k + 1) * moves], length, 7)[0]):
                    targets[k, c] = value

    return kernel


def final_kernel(sizes, slots, moves):
    boxes = shell(sizes)
    images = image_list(boxes)
    tile = moves
    halves = slots // LANES
    edge = box_length(slots)
    length = edge / CUTOFF

    def kernel(
        recv, frames, ahi, alo, bhi, blo, own, perm, shift, source, arrive, hits, targets,
        staying, arrivals, lhs, sums, acc, table, out_stay, out_come, out_sems,
    ):
        cell = own_cell()
        places = around(cell, CENTERS[0], boxes, sizes)
        build_lhs(lhs, recv, frames, places, images, slots)
        fill_table(table, cell, boxes, sizes)
        lane = lax.broadcasted_iota(jnp.int32, (1, LANES), 1)
        origin = [linear(cell, [-step for step in unit], sizes) for unit in UNITS]
        blank = jnp.zeros((5, slots), F32)
        blocks = []
        for k in range(6):
            for a in range(3):
                blocks.append(
                    jnp.concatenate([recv[origin[k], a * halves + h] for h in range(halves)], axis=1)
                )
            blocks.append(blank)
        taken = pick(jnp.concatenate(blocks, axis=0), hits[...])
        moment = jnp.zeros((8, LANES), F32)
        for k in range(6):
            moment = jnp.where(lane // moves == k, taken[8 * k : 8 * k + 8], moment)
        got = arrive[0:8]
        extra = arrive[8:16]
        present = extra[0:1] >= 0.0
        acc[...] = jnp.zeros(acc.shape, F32)
        steps = [len(images) // 6 * slots, len(boxes) // 6 * slots]
        for which, (high, low, count) in enumerate(((ahi, alo, len(images)), (bhi, blo, len(boxes)))):
            sums[which] = jnp.zeros((48, slots), F32)
            if count * slots > 6 * steps[which]:
                sums[which] = product(lhs, high, low, slice(6 * steps[which], count * slots))

        def incoming(k, carry):
            for which, (high, low) in enumerate(((ahi, alo), (bhi, blo))):
                part = pl.ds(pl.multiple_of(k * steps[which], LANES), steps[which])
                sums[which] = sums[which] + product(lhs, high, low, part)
            at = pl.ds(pl.multiple_of(k * tile, tile), tile)
            wide = [targets[k, c] for c in range(7)]
            shifted = [{-1: wide[a] + length, 0: wide[a], 1: wide[a] - length} for a in range(3)]
            fields = [jnp.zeros((tile, LANES), F32)] * 3
            for n, box in enumerate(boxes):
                spot = table[(k + 1) * len(boxes) + n]
                for half in range(halves):
                    row = reader(source, spot, half, tile)
                    mu = [
                        jnp.broadcast_to(recv[spot, a * halves + half], (tile, LANES))
                        for a in range(3)
                    ]
                    deltas = offsets(wide, shifted, row, box, length)
                    dist_sq = norm(deltas)
                    if is_center(box):
                        ids = lax.broadcasted_iota(jnp.int32, (tile, LANES), 1) + half * LANES
                        keep = wide[6] != ids.astype(F32)
                        dist_sq = jnp.where(keep, dist_sq, 1.0)
                    inverse, half_x, tanh, base = terms(wide, dist_sq, row)
                    direct = base * tanh
                    radial = (inverse * inverse) * (direct - half_x * (base - direct))
                    if is_center(box):
                        direct = jnp.where(keep, direct, 0.0)
                        radial = jnp.where(keep, radial, 0.0)
                    pull = jnp.where(wide[5] != row(6), direct, 0.0) * row(3)
                    pull = pull + (3.0 * radial) * (deltas[0] * mu[0] + deltas[1] * mu[1] + deltas[2] * mu[2])
                    fields = [fields[a] + (pull * deltas[a] - direct * mu[a]) for a in range(3)]
            for a in range(3):
                acc[a, at, :] = fields[a]
            return carry

        lax.fori_loop(0, 6, incoming, 0)
        field = induced_rows(sums[0], sums[1], own, perm, slots)
        remain = own[12:13] > 0.5
        fast = [own[8 + a : 9 + a] + own[15:16] * field[a] for a in range(3)]
        place = [own[a : a + 1] + TIMESTEP * fast[a] / edge for a in range(3)]
        drude = [shift[a : a + 1] for a in range(3)]
        for r, row in enumerate(place + fast + drude):
            out_stay[r] = jnp.where(remain, row, 0.0)
        early = pltpu.make_async_copy(out_stay, staying, out_sems.at[0])
        early.start()

        pull = rows_of([acc[a] for a in range(3)])
        q = got[3:4]
        qd = got[4:5]
        mass = jnp.where(present, extra[4:5], 1.0)
        gain = KICK * q / mass
        fast = [extra[1 + a : 2 + a] + gain * pull[a] for a in range(3)]
        place = [got[a : a + 1] + TIMESTEP * fast[a] / edge for a in range(3)]
        for k, unit in enumerate(UNITS):
            for a in range(3):
                if unit[a]:
                    place[a] = place[a] - jnp.where(lane // moves == k, float(unit[a]), 0.0)
        safe = jnp.where(present, qd, -1.0) * MOMENT
        drude = [moment[a : a + 1] / safe for a in range(3)]
        record = place + fast + drude + [q, qd, got[5:6], got[6:7], mass]
        for r, row in enumerate(record):
            out_come[r] = jnp.where(present, row, 0.0)[:, 0 : 6 * moves]
        late = pltpu.make_async_copy(out_come, arrivals, out_sems.at[1])
        late.start()
        early.wait()
        late.wait()

    return kernel


def solution(mesh):
    sizes = tuple(mesh.shape[axis] for axis in AXES)
    devices = int(np.prod(sizes))
    boxes = shell(sizes)
    count_boxes = len(boxes)
    count_images = len(image_list(boxes))
    padded_boxes = -(-count_boxes // 16) * 16

    def local(fractions, velocity, charge, drude_charge, screening, labels, masses, counts, leaving):
        slots = charge.shape[-1]
        moves = leaving.shape[-1]
        exchange = lambda block: lax.all_to_all(block, AXES, 0, 0)
        shape = lambda *dims: jax.ShapeDtypeStruct(dims, F32)
        half = lambda *dims: jax.ShapeDtypeStruct(dims, BF16)
        hbm = lambda x: pltpu.with_memory_space_constraint(x, pltpu.HBM)
        moment_shape = (devices, 3 * (slots // LANES), 1, LANES)
        dma = pltpu.SemaphoreType.DMA

        def call(kernel, in_specs, outs, out_specs, scratch, flops, limit):
            return pl.pallas_call(
                kernel,
                in_specs=in_specs,
                out_shape=outs,
                out_specs=out_specs,
                scratch_shapes=scratch,
                compiler_params=pltpu.CompilerParams(vmem_limit_bytes=limit),
                cost_estimate=pl.CostEstimate(flops=flops, bytes_accessed=1 << 20, transcendentals=0),
            )

        flat = [
            fractions.reshape(3, 1, slots),
            velocity.reshape(3, 1, slots),
            charge.reshape(1, slots),
            drude_charge.reshape(1, slots),
            screening.reshape(1, slots),
            labels.reshape(1, slots),
            masses.reshape(1, slots),
            leaving.reshape(6, 1, moves),
        ]
        send, own = call(
            pack_kernel(sizes, slots, moves),
            [smem()] + [anywhere()] * 8,
            (shape(devices, 8, slots), shape(16, slots)),
            (vmem(), vmem()),
            [VMEM(array.shape, array.dtype) for array in flat] + [dma((8,))],
            1 << 20,
            8 << 20,
        )(counts.reshape(1), *[hbm(x) for x in flat])
        first = exchange(send)
        outs = (
            shape(devices, 8, slots),
            shape(count_images, 8, slots),
            half(count_images * slots, slots),
            half(count_images * slots, slots),
            half(count_boxes * slots, slots),
            half(count_boxes * slots, slots),
            shape(3, slots),
            shape(*moment_shape),
        )
        source, frames, ahi, alo, bhi, blo, perm, moments = call(
            field_kernel(sizes, slots, 32),
            [vmem()] * 2,
            outs,
            (vmem(),) * len(outs),
            [
                VMEM((padded_boxes, 8, slots), F32),
                VMEM((slots, padded_boxes * 8), F32),
                VMEM((3, 8, slots), F32),
                VMEM((7, 32, LANES), F32),
            ],
            1 << 25,
            8 << 20,
        )(first, own)
        got = exchange(moments)
        tensors = (frames, ahi, alo, bhi, blo, own, perm)
        lhs = VMEM((48, count_images * slots), BF16)
        for step in range(ITERS - 1):
            prepare = step == ITERS - 2
            outs = (shape(*moment_shape), shape(3, slots))
            if prepare:
                outs = outs + (shape(16, LANES), half(slots, LANES), shape(6, 7, moves, LANES))
            moments, shift, *arriving = call(
                induced_kernel(sizes, slots, moves, prepare),
                [vmem()] * (9 if prepare else 8),
                outs,
                (vmem(),) * len(outs),
                [lhs],
                1 << 24,
                4 << 20,
            )(got, *tensors, *((first,) if prepare else ()))
            got = exchange(moments)
        staying, arrivals = call(
            final_kernel(sizes, slots, moves),
            [vmem()] * 13,
            (pltpu.HBM((9, 1, slots), F32), pltpu.HBM((14, 1, 6 * moves), F32)),
            (anywhere(), anywhere()),
            [
                lhs,
                VMEM((2, 48, slots), F32),
                VMEM((3, LANES, LANES), F32),
                pltpu.SMEM((len(CENTERS) * count_boxes,), jnp.int32),
                VMEM((9, 1, slots), F32),
                VMEM((14, 1, 6 * moves), F32),
                dma((2,)),
            ],
            1 << 24,
            8 << 20,
        )(got, *tensors, shift, source, *arriving)
        return staying.reshape(1, 1, 1, 9, slots), arrivals.reshape(1, 1, 1, 14, 6 * moves)

    box = P("gx", "gy", "gz", None)
    rows = P("gx", "gy", "gz", None, None)
    return jax.shard_map(
        local,
        mesh=mesh,
        in_specs=(rows, rows, box, box, box, box, box, P("gx", "gy", "gz"), rows),
        out_specs=(rows, rows),
        check_vma=False,
    )
```

```python
import itertools

import jax
import jax.numpy as jnp
import numpy as np
from jax import lax
from jax.experimental import pallas as pl
from jax.experimental.pallas import tpu as pltpu
from jax.sharding import PartitionSpec as P

ITERS = 3
CUTOFF = 12.0
DRUDE_GAIN = 0.3320636
KICK = 0.002 * 418.4 * 332.0636
TIMESTEP = 0.002
UNITS = ((1, 0, 0), (-1, 0, 0), (0, 1, 0), (0, -1, 0), (0, 0, 1), (0, 0, -1))
AXES = ("gx", "gy", "gz")
LANES = 128
CENTERS = ((0, 0, 0),) + tuple(tuple(-step for step in unit) for unit in UNITS)
MOMENT = 2.0 / CUTOFF**3
F32 = jnp.float32
BF16 = jnp.bfloat16
VMEM = pltpu.VMEM


def vmem():
    return pl.BlockSpec(memory_space=pltpu.VMEM)


def smem():
    return pl.BlockSpec(memory_space=pltpu.SMEM)


def anywhere():
    return pl.BlockSpec(memory_space=pltpu.HBM)


def box_length(slots):
    return max(12.0, (10.0 * slots) ** (1.0 / 3.0))


def axis_steps(count):
    return ((0, False), (1, True)) if count == 2 else ((-1, False), (0, False), (1, False))


def shell(sizes):
    return list(itertools.product(*[axis_steps(count) for count in sizes]))


def own_cell():
    return [lax.axis_index(axis) for axis in AXES]


def linear(cell, steps, sizes):
    value = 0
    for coordinate, step, count in zip(cell, steps, sizes):
        value = value * count + (coordinate + (step % count)) % count
    return value


def around(cell, center, boxes, sizes):
    return [linear(cell, [center[a] + box[a][0] for a in range(3)], sizes) for box in boxes]


def fill_table(table, cell, boxes, sizes):
    for g, center in enumerate(CENTERS):
        for n, place in enumerate(around(cell, center, boxes, sizes)):
            table[g * len(boxes) + n] = place


def pieces_of(values):
    pieces = []
    for _ in range(3):
        piece = values.astype(BF16).astype(F32)
        pieces.append(piece)
        values = values - piece
    return pieces


def pick(blocks, hit):
    count = blocks.shape[0]
    stacked = jnp.concatenate(pieces_of(blocks), axis=0).astype(BF16)
    got = jnp.dot(stacked, hit, preferred_element_type=F32)
    return (got[0:count] + got[count : 2 * count]) + got[2 * count :]


def pack_kernel(sizes, slots, moves):
    devices = int(np.prod(sizes))

    def kernel(*refs):
        count, inputs, (send, own), staged, sems = refs[0], refs[1:9], refs[9:11], refs[11:19], refs[19]
        copies = [pltpu.make_async_copy(inputs[i], staged[i], sems.at[i]) for i in range(8)]
        for copy in copies:
            copy.start()
        for copy in copies:
            copy.wait()
        frac, vel, charge, drude, screen, label, mass, leaving = staged
        cell = own_cell()
        lane = lax.broadcasted_iota(jnp.int32, (1, slots), 1)
        live = lane < count[0]
        fr = jnp.concatenate([frac[a] for a in range(3)], axis=0)
        ve = jnp.concatenate([vel[a] for a in range(3)], axis=0)
        q = jnp.where(live, charge[...], 0.0)
        qd = jnp.where(live, drude[...], -1.0)
        sc = screen[...]
        lb = label[...].astype(F32)
        ms = mass[...]
        lv = jnp.concatenate([leaving[k].astype(F32) for k in range(6)], axis=0)
        lv = jnp.concatenate([lv, jnp.full((2, moves), -1.0, F32)], axis=0)
        spread = (
            lax.broadcasted_iota(jnp.int32, (moves, LANES), 1) % moves
            == lax.broadcasted_iota(jnp.int32, (moves, LANES), 0)
        ).astype(F32)
        repeated = jnp.dot(lv.astype(BF16), spread.astype(BF16), preferred_element_type=F32)
        slot_col = lax.broadcasted_iota(jnp.int32, (slots, LANES), 0).astype(F32)
        values = jnp.concatenate([ve, ms, jnp.zeros((4, slots), F32)], axis=0)
        field = lax.broadcasted_iota(jnp.int32, (8, LANES), 1) // moves - 1
        wanted = field == lax.broadcasted_iota(jnp.int32, (8, LANES), 0)
        first = lax.broadcasted_iota(jnp.int32, (1, LANES), 1) < moves
        statics = jnp.concatenate([fr, q, qd, sc, lb, jnp.zeros((1, slots), F32)], axis=0)
        send[...] = jnp.broadcast_to(statics[None], (devices, 8, slots))
        hits = jnp.concatenate(
            [(slot_col == repeated[k : k + 1]).astype(F32).astype(BF16) for k in range(6)], axis=1
        )
        picked = pick(values, hits)
        for k, unit in enumerate(UNITS):
            mine = picked[:, k * LANES : (k + 1) * LANES]
            row = jnp.sum(jnp.where(wanted, mine, 0.0), axis=0, keepdims=True)
            row = jnp.where(first, repeated[k : k + 1], row)
            side = (k % 2) * LANES
            send[linear(cell, unit, sizes), 7:8, side : side + LANES] = row
        ones = jnp.ones((16, 6 * LANES), BF16)
        departed = lax.dot_general(ones, hits, (((1,), (1,)), ((), ())), preferred_element_type=F32)[0:1]
        alive = live.astype(F32)
        gain = jnp.where(live, DRUDE_GAIN * qd, 0.0)
        own[...] = jnp.concatenate(
            [fr, q, qd, sc, lb, ms, ve, alive, jnp.where(departed > 0.5, 0.0, alive)]
            + [MOMENT * (gain * qd), gain, KICK * q / ms],
            axis=0,
        )

    return kernel


def columns(rows):
    lanes = rows.shape[1]
    padded = jnp.concatenate([rows, jnp.zeros((LANES - rows.shape[0], lanes), F32)], axis=0)
    return padded.T


def derived(fr, qd, sc, length):
    root = (DRUDE_GAIN**-0.5) / jnp.abs(qd)
    return fr * length, root, (0.25 * CUTOFF**3) * sc * root


def target_of(block, length, count):
    rows = block.shape[0]
    wide = [jnp.broadcast_to(block[:, c : c + 1], (rows, LANES)) for c in range(count)]
    shifted = [{-1: wide[a] + length, 0: wide[a], 1: wide[a] - length} for a in range(3)]
    return wide, shifted


def reader(source, place, half, rows):
    lanes = slice(half * LANES, (half + 1) * LANES)
    return lambda c: jnp.broadcast_to(source[place, c : c + 1, lanes], (rows, LANES))


def offsets(wide, shifted, row, box, length):
    deltas = []
    for a in range(3):
        step, nearest = box[a]
        if nearest:
            raw = wide[a] - row(a)
            deltas.append(raw - jnp.where(raw > 0.0, length, -length))
        else:
            deltas.append(shifted[a][step] - row(a))
    return deltas


def norm(deltas):
    return deltas[0] * deltas[0] + deltas[1] * deltas[1] + deltas[2] * deltas[2]


def terms(wide, dist_sq, row):
    inverse = lax.rsqrt(dist_sq)
    fade = inverse * jnp.maximum(1.0 - dist_sq, 0.0)
    half_x = (wide[3] * row(5) + wide[4] * row(4)) * (dist_sq * (dist_sq * inverse))
    tanh = jnp.tanh(half_x)
    root = fade * lax.rsqrt(1.0 + tanh)
    base = (root * root) * inverse
    return inverse, half_x, tanh, base


def charge_sum(fields, wide, deltas, direct, row):
    weight = jnp.where(wide[5] != row(6), direct, 0.0) * row(3)
    return [fields[a] + weight * deltas[a] for a in range(3)]


def image_list(boxes):
    first, rest = [], []
    for n, box in enumerate(boxes):
        combos = list(itertools.product(*[(1, -1) if nearest else (step,) for step, nearest in box]))
        first.append((n, combos[0]))
        rest.extend((n, combo) for combo in combos[1:])
    return first + rest


def is_center(box):
    return all(step == 0 for step, _ in box)


def rows_of(parts):
    return [jnp.sum(part.T, axis=0, keepdims=True) for part in parts]


def send_moments(send, moments, slots):
    halves = slots // LANES
    for a in range(3):
        for h in range(halves):
            row = moments[a][:, h * LANES : (h + 1) * LANES]
            send[:, a * halves + h] = jnp.broadcast_to(row[None], (send.shape[0], 1, LANES))


def split(values, high, low, spot):
    high[spot, :] = values.astype(BF16)
    low[spot, :] = (values - high[spot, :].astype(F32)).astype(BF16)


def field_kernel(sizes, slots, tile):
    boxes = shell(sizes)
    images = image_list(boxes)
    length = box_length(slots) / CUTOFF

    def kernel(recv, own, source, frames, ahi, alo, bhi, blo, perm, send, chosen, cols, acc, ready):
        fr, root, part = derived(recv[:, 0:3, :], recv[:, 4:5, :], recv[:, 5:6, :], length)
        source[:, 0:3, :] = fr
        source[:, 3:4, :] = (2.0 / CUTOFF**2) * recv[:, 3:4, :]
        source[:, 4:5, :] = root
        source[:, 5:6, :] = part
        source[:, 6:8, :] = recv[:, 6:8, :]
        places = around(own_cell(), CENTERS[0], boxes, sizes)
        for n in range(len(boxes)):
            chosen[n] = source[places[n]]
        for n in range(len(boxes), chosen.shape[0]):
            chosen[n] = jnp.zeros((8, slots), F32)
        group = LANES // 8
        for g in range(chosen.shape[0] // group):
            cols[:, g * LANES : (g + 1) * LANES] = chosen[g * group : (g + 1) * group].reshape(LANES, slots).T
        one = jnp.ones((1, slots), F32)
        for m, (n, step) in enumerate(images):
            spots = [chosen[n, a : a + 1, :] + (step[a] - 0.5) * length for a in range(3)]
            frames[m] = jnp.concatenate(spots + [one] + spots + [one], axis=0)
        fr, root, part = derived(own[0:3], own[4:5], own[5:6], length)
        wide = [jnp.broadcast_to(row, (tile, slots)) for row in (fr[0:1], fr[1:2], fr[2:3], root, part, own[6:7])]
        acc[...] = jnp.zeros(acc.shape, F32)

        def body(t, carry):
            at = pl.ds(pl.multiple_of(t * tile, tile), tile)
            block = cols[at, :]
            after = pl.ds(pl.multiple_of(jnp.minimum(t + 1, slots // tile - 1) * tile, tile), tile)
            upcoming = cols[after, :]
            fields = [acc[a] for a in range(3)]
            for n, box in enumerate(boxes):
                if n == 0:
                    row = lambda c: jnp.concatenate([ready[c]] * (slots // LANES), axis=1)
                else:
                    row = lambda c: jnp.broadcast_to(block[:, n * 8 + c : n * 8 + c + 1], (tile, slots))
                deltas, ahead = [], []
                for a in range(3):
                    step, nearest = box[a]
                    raw = wide[a] - row(a) if nearest or not step else (wide[a] - step * length) - row(a)
                    if nearest:
                        ahead.append((a, raw > 0.0))
                        raw = raw - jnp.where(ahead[-1][1], length, -length)
                    deltas.append(raw)
                dist_sq = norm(deltas)
                if is_center(box):
                    target = lax.broadcasted_iota(jnp.int32, (tile, slots), 1)
                    keep = target != lax.broadcasted_iota(jnp.int32, (tile, slots), 0) + t * tile
                    dist_sq = jnp.where(keep, dist_sq, 1.0)
                inverse, half_x, tanh, base = terms(wide, dist_sq, row)
                direct = base * tanh
                weight = jnp.where(wide[5] != row(6), direct, 0.0) * row(3)
                fields = [
                    fields[a] + jnp.sum((weight * deltas[a]).reshape(tile // 8, 8, slots), axis=0)
                    for a in range(3)
                ]
                radial = (inverse * inverse) * (direct - half_x * (base - direct))
                if is_center(box):
                    direct = jnp.where(keep, direct, 0.0)
                    radial = jnp.where(keep, radial, 0.0)
                spot = pl.ds(pl.multiple_of(n * slots + t * tile, tile), tile)
                split(direct, bhi, blo, spot)
                for m, (owner, step) in enumerate(images):
                    if owner != n:
                        continue
                    part = radial
                    for a, side in ahead:
                        part = jnp.where(side, part, 0.0) if step[a] > 0 else jnp.where(side, 0.0, part)
                    spot = pl.ds(pl.multiple_of(m * slots + t * tile, tile), tile)
                    split(part, ahi, alo, spot)
            for a in range(3):
                acc[a] = fields[a]
            for c in range(7):
                ready[c] = jnp.broadcast_to(upcoming[:, c : c + 1], (tile, LANES))
            return carry

        for c in range(7):
            ready[c] = jnp.broadcast_to(cols[0:tile, c : c + 1], (tile, LANES))

        lax.fori_loop(0, slots // tile, body, 0, unroll=2)
        rows = [jnp.sum(acc[a], axis=0, keepdims=True) for a in range(3)]
        perm[...] = jnp.concatenate(rows, axis=0)
        send_moments(send, [own[13:14] * row for row in rows], slots)

    return kernel


def build_lhs(lhs, recv, frames, places, images, slots):
    halves = slots // LANES
    upper = lax.broadcasted_iota(jnp.int32, (8, slots), 0) < 4
    known = {}
    for m, (n, _) in enumerate(images):
        if n not in known:
            known[n] = [
                jnp.concatenate(
                    [recv[places[n], a * halves + h] for h in range(halves)], axis=1
                )
                for a in range(3)
            ]
        mu = known[n]
        along = frames[m, 0:1, :] * mu[0] + frames[m, 1:2, :] * mu[1] + frames[m, 2:3, :] * mu[2]
        frame = frames[m]
        whole = lambda row: jnp.broadcast_to(row, (8, slots))
        value = jnp.concatenate(
            [
                frame * jnp.where(upper, whole(mu[0]), whole(mu[1])),
                frame * jnp.where(upper, whole(mu[2]), whole(along)),
            ],
            axis=0,
        )
        lanes = slice(m * slots, (m + 1) * slots)
        for piece in range(3):
            high = value.astype(BF16)
            lhs[piece * 16 : (piece + 1) * 16, lanes] = high
            value = value - high.astype(F32)


def product(lhs, high, low, at):
    left = lhs[:, at]
    dot = lambda right: jnp.dot(left, right[at, :], preferred_element_type=F32)
    return dot(high) + dot(low)


def induced_rows(tensor, plain, own, perm, slots):
    length = box_length(slots) / CUTOFF
    tensor = 3.0 * (tensor[0:16] + (tensor[16:32] + tensor[32:48]))
    plain = plain[0:16] + (plain[16:32] + plain[32:48])
    spot = [(own[a : a + 1] - 0.5) * length for a in range(3)]
    first = [tensor[4 * a + 3 : 4 * a + 4] for a in range(3)]
    along = spot[0] * first[0] + spot[1] * first[1] + spot[2] * first[2] - tensor[15:16]
    rows = []
    for a in range(3):
        mixed = sum(tensor[4 * b + a : 4 * b + a + 1] * spot[b] for b in range(3))
        value = (spot[a] * along - mixed) + tensor[12 + a : 13 + a]
        rows.append(perm[a : a + 1] + (value - plain[4 * a + 3 : 4 * a + 4]))
    return rows


def arrival_records(first_recv, origin, moves, slots):
    lane = lax.broadcasted_iota(jnp.int32, (1, LANES), 1)
    extra = jnp.full((8, LANES), -1.0, F32)
    for k in range(6):
        side = (k % 2) * LANES
        row = first_recv[origin[k], 7:8, side : side + LANES]
        row = jnp.broadcast_to(row, (8, LANES))
        fields = [pltpu.roll(row, (k * moves - c * moves) % LANES, 1)[0:1] for c in range(5)]
        block = jnp.concatenate(fields + [extra[0:3]], axis=0)
        extra = jnp.where(lane // moves == k, block, extra)
    slot = extra[0:1]
    slot_col = lax.broadcasted_iota(jnp.int32, (slots, LANES), 0).astype(F32)
    hit = (slot_col == slot).astype(F32).astype(BF16)
    taken = pick(jnp.concatenate([first_recv[origin[k]] for k in range(6)], axis=0), hit)
    got = jnp.zeros((8, LANES), F32)
    for k in range(6):
        got = jnp.where(lane // moves == k, taken[8 * k : 8 * k + 8], got)
    return got, extra, hit


def induced_kernel(sizes, slots, moves, prepare):
    boxes = shell(sizes)
    images = image_list(boxes)
    length = box_length(slots) / CUTOFF

    def kernel(recv, frames, ahi, alo, bhi, blo, own, perm, *rest):
        if prepare:
            first_recv, send, shift, arrive, hits, targets, lhs = rest
        else:
            send, shift, lhs = rest
        cell = own_cell()
        places = around(cell, CENTERS[0], boxes, sizes)
        build_lhs(lhs, recv, frames, places, images, slots)
        tensor = product(lhs, ahi, alo, slice(0, len(images) * slots))
        plain = product(lhs, bhi, blo, slice(0, len(boxes) * slots))
        rows = induced_rows(tensor, plain, own, perm, slots)
        shift[...] = jnp.concatenate([own[14:15] * row for row in rows], axis=0)
        send_moments(send, [own[13:14] * row for row in rows], slots)
        if prepare:
            origin = [linear(cell, [-step for step in unit], sizes) for unit in UNITS]
            got, extra, hit = arrival_records(first_recv, origin, moves, slots)
            arrive[0:8] = got
            arrive[8:16] = extra
            hits[...] = hit
            slot = extra[0:1]
            fr, root, part = derived(got[0:3], jnp.where(slot >= 0.0, got[4:5], -1.0), got[5:6], length)
            cols = columns(jnp.concatenate([fr, root, part, got[6:7], slot, slot], axis=0))
            for k in range(6):
                for c, value in enumerate(target_of(cols[k * moves : (k + 1) * moves], length, 7)[0]):
                    targets[k, c] = value

    return kernel


def final_kernel(sizes, slots, moves):
    boxes = shell(sizes)
    images = image_list(boxes)
    tile = moves
    halves = slots // LANES
    edge = box_length(slots)
    length = edge / CUTOFF

    def kernel(
        recv, frames, ahi, alo, bhi, blo, own, perm, shift, source, arrive, hits, targets,
        staying, arrivals, lhs, sums, acc, table, out_stay, out_come, out_sems,
    ):
        cell = own_cell()
        places = around(cell, CENTERS[0], boxes, sizes)
        build_lhs(lhs, recv, frames, places, images, slots)
        fill_table(table, cell, boxes, sizes)
        lane = lax.broadcasted_iota(jnp.int32, (1, LANES), 1)
        origin = [linear(cell, [-step for step in unit], sizes) for unit in UNITS]
        blank = jnp.zeros((5, slots), F32)
        blocks = []
        for k in range(6):
            for a in range(3):
                blocks.append(
                    jnp.concatenate([recv[origin[k], a * halves + h] for h in range(halves)], axis=1)
                )
            blocks.append(blank)
        taken = pick(jnp.concatenate(blocks, axis=0), hits[...])
        moment = jnp.zeros((8, LANES), F32)
        for k in range(6):
            moment = jnp.where(lane // moves == k, taken[8 * k : 8 * k + 8], moment)
        got = arrive[0:8]
        extra = arrive[8:16]
        present = extra[0:1] >= 0.0
        acc[...] = jnp.zeros(acc.shape, F32)
        steps = [len(images) // 6 * slots, len(boxes) // 6 * slots]
        for which, (high, low, count) in enumerate(((ahi, alo, len(images)), (bhi, blo, len(boxes)))):
            sums[which] = jnp.zeros((48, slots), F32)
            if count * slots > 6 * steps[which]:
                sums[which] = product(lhs, high, low, slice(6 * steps[which], count * slots))

        def incoming(k, carry):
            for which, (high, low) in enumerate(((ahi, alo), (bhi, blo))):
                part = pl.ds(pl.multiple_of(k * steps[which], LANES), steps[which])
                sums[which] = sums[which] + product(lhs, high, low, part)
            at = pl.ds(pl.multiple_of(k * tile, tile), tile)
            wide = [targets[k, c] for c in range(7)]
            shifted = [{-1: wide[a] + length, 0: wide[a], 1: wide[a] - length} for a in range(3)]
            fields = [jnp.zeros((tile, LANES), F32)] * 3
            for n, box in enumerate(boxes):
                spot = table[(k + 1) * len(boxes) + n]
                for half in range(halves):
                    row = reader(source, spot, half, tile)
                    mu = [
                        jnp.broadcast_to(recv[spot, a * halves + half], (tile, LANES))
                        for a in range(3)
                    ]
                    deltas = offsets(wide, shifted, row, box, length)
                    dist_sq = norm(deltas)
                    if is_center(box):
                        ids = lax.broadcasted_iota(jnp.int32, (tile, LANES), 1) + half * LANES
                        keep = wide[6] != ids.astype(F32)
                        dist_sq = jnp.where(keep, dist_sq, 1.0)
                    inverse, half_x, tanh, base = terms(wide, dist_sq, row)
                    direct = base * tanh
                    radial = (inverse * inverse) * (direct - half_x * (base - direct))
                    if is_center(box):
                        direct = jnp.where(keep, direct, 0.0)
                        radial = jnp.where(keep, radial, 0.0)
                    pull = jnp.where(wide[5] != row(6), direct, 0.0) * row(3)
                    pull = pull + (3.0 * radial) * (deltas[0] * mu[0] + deltas[1] * mu[1] + deltas[2] * mu[2])
                    fields = [fields[a] + (pull * deltas[a] - direct * mu[a]) for a in range(3)]
            for a in range(3):
                acc[a, at, :] = fields[a]
            return carry

        lax.fori_loop(0, 6, incoming, 0)
        field = induced_rows(sums[0], sums[1], own, perm, slots)
        remain = own[12:13] > 0.5
        fast = [own[8 + a : 9 + a] + own[15:16] * field[a] for a in range(3)]
        place = [own[a : a + 1] + TIMESTEP * fast[a] / edge for a in range(3)]
        drude = [shift[a : a + 1] for a in range(3)]
        for r, row in enumerate(place + fast + drude):
            out_stay[r] = jnp.where(remain, row, 0.0)
        early = pltpu.make_async_copy(out_stay, staying, out_sems.at[0])
        early.start()

        pull = rows_of([acc[a] for a in range(3)])
        q = got[3:4]
        qd = got[4:5]
        mass = jnp.where(present, extra[4:5], 1.0)
        gain = KICK * q / mass
        fast = [extra[1 + a : 2 + a] + gain * pull[a] for a in range(3)]
        place = [got[a : a + 1] + TIMESTEP * fast[a] / edge for a in range(3)]
        for k, unit in enumerate(UNITS):
            for a in range(3):
                if unit[a]:
                    place[a] = place[a] - jnp.where(lane // moves == k, float(unit[a]), 0.0)
        safe = jnp.where(present, qd, -1.0) * MOMENT
        drude = [moment[a : a + 1] / safe for a in range(3)]
        record = place + fast + drude + [q, qd, got[5:6], got[6:7], mass]
        for r, row in enumerate(record):
            out_come[r] = jnp.where(present, row, 0.0)[:, 0 : 6 * moves]
        late = pltpu.make_async_copy(out_come, arrivals, out_sems.at[1])
        late.start()
        early.wait()
        late.wait()

    return kernel


def solution(mesh):
    sizes = tuple(mesh.shape[axis] for axis in AXES)
    devices = int(np.prod(sizes))
    boxes = shell(sizes)
    count_boxes = len(boxes)
    count_images = len(image_list(boxes))
    padded_boxes = -(-count_boxes // 16) * 16

    def local(fractions, velocity, charge, drude_charge, screening, labels, masses, counts, leaving):
        slots = charge.shape[-1]
        moves = leaving.shape[-1]
        exchange = lambda block: lax.all_to_all(block, AXES, 0, 0)
        shape = lambda *dims: jax.ShapeDtypeStruct(dims, F32)
        half = lambda *dims: jax.ShapeDtypeStruct(dims, BF16)
        hbm = lambda x: pltpu.with_memory_space_constraint(x, pltpu.HBM)
        moment_shape = (devices, 3 * (slots // LANES), 1, LANES)
        dma = pltpu.SemaphoreType.DMA

        def call(kernel, in_specs, outs, out_specs, scratch, flops, limit):
            return pl.pallas_call(
                kernel,
                in_specs=in_specs,
                out_shape=outs,
                out_specs=out_specs,
                scratch_shapes=scratch,
                compiler_params=pltpu.CompilerParams(vmem_limit_bytes=limit),
                cost_estimate=pl.CostEstimate(flops=flops, bytes_accessed=1 << 20, transcendentals=0),
            )

        flat = [
            fractions.reshape(3, 1, slots),
            velocity.reshape(3, 1, slots),
            charge.reshape(1, slots),
            drude_charge.reshape(1, slots),
            screening.reshape(1, slots),
            labels.reshape(1, slots),
            masses.reshape(1, slots),
            leaving.reshape(6, 1, moves),
        ]
        send, own = call(
            pack_kernel(sizes, slots, moves),
            [smem()] + [anywhere()] * 8,
            (shape(devices, 8, slots), shape(16, slots)),
            (vmem(), vmem()),
            [VMEM(array.shape, array.dtype) for array in flat] + [dma((8,))],
            1 << 20,
            8 << 20,
        )(counts.reshape(1), *[hbm(x) for x in flat])
        first = exchange(send)
        outs = (
            shape(devices, 8, slots),
            shape(count_images, 8, slots),
            half(count_images * slots, slots),
            half(count_images * slots, slots),
            half(count_boxes * slots, slots),
            half(count_boxes * slots, slots),
            shape(3, slots),
            shape(*moment_shape),
        )
        source, frames, ahi, alo, bhi, blo, perm, moments = call(
            field_kernel(sizes, slots, 32),
            [vmem()] * 2,
            outs,
            (vmem(),) * len(outs),
            [
                VMEM((padded_boxes, 8, slots), F32),
                VMEM((slots, padded_boxes * 8), F32),
                VMEM((3, 8, slots), F32),
                VMEM((7, 32, LANES), F32),
            ],
            1 << 25,
            16 << 20,
        )(first, own)
        got = exchange(moments)
        tensors = (frames, ahi, alo, bhi, blo, own, perm)
        lhs = VMEM((48, count_images * slots), BF16)
        for step in range(ITERS - 1):
            prepare = step == ITERS - 2
            outs = (shape(*moment_shape), shape(3, slots))
            if prepare:
                outs = outs + (shape(16, LANES), half(slots, LANES), shape(6, 7, moves, LANES))
            moments, shift, *arriving = call(
                induced_kernel(sizes, slots, moves, prepare),
                [vmem()] * (9 if prepare else 8),
                outs,
                (vmem(),) * len(outs),
                [lhs],
                1 << 24,
                4 << 20,
            )(got, *tensors, *((first,) if prepare else ()))
            got = exchange(moments)
        staying, arrivals = call(
            final_kernel(sizes, slots, moves),
            [vmem()] * 13,
            (pltpu.HBM((9, 1, slots), F32), pltpu.HBM((14, 1, 6 * moves), F32)),
            (anywhere(), anywhere()),
            [
                lhs,
                VMEM((2, 48, slots), F32),
                VMEM((3, LANES, LANES), F32),
                pltpu.SMEM((len(CENTERS) * count_boxes,), jnp.int32),
                VMEM((9, 1, slots), F32),
                VMEM((14, 1, 6 * moves), F32),
                dma((2,)),
            ],
            1 << 24,
            8 << 20,
        )(got, *tensors, shift, source, *arriving)
        return staying.reshape(1, 1, 1, 9, slots), arrivals.reshape(1, 1, 1, 14, 6 * moves)

    box = P("gx", "gy", "gz", None)
    rows = P("gx", "gy", "gz", None, None)
    return jax.shard_map(
        local,
        mesh=mesh,
        in_specs=(rows, rows, box, box, box, box, box, P("gx", "gy", "gz"), rows),
        out_specs=(rows, rows),
        check_vma=False,
    )
```
